32 devices in a mesh: blk: 8 (over z, x), span: 4 (over y, core).
Axes of the slice: x: 2, y: 2, z: 4, core: 2. Of those that a mesh axis runs over, the one named last changes fastest.
Arguments:
- fields: float32 [5, 125, 16384], P(None, None, ('blk', 'span')), may hold values from -6 to 6
- section_store: float32 [5, 125, 16384], P(None, None, ('blk', 'span')), may hold values from -6 to 6
- mean_velocity: float32 [3, 125, 16384], P(None, None, ('blk', 'span')), may hold values from -0.6 to 0.6
- sound_speed: float32 [125, 16384], P(None, ('blk', 'span')), may hold values from 0.7 to 1.5
- element_slot: int32 [16384], P(('blk', 'span')), may hold values from 0 to 511, as said below
- face_turn: int32 [8, 16], P('blk', 'span'), may hold values from 0 to 7
- rotor_offset: int32 [16], P('span'), may hold values from 0 to 7
Outputs:
- fields_next: float32 [5, 125, 16384], P(None, None, ('blk', 'span'))
- store_next: float32 [5, 125, 16384], P(None, None, ('blk', 'span'))
The draws below stay inside these ranges and needn't reach their ends.
Inputs may be any that keep to these rules, and one draw needn't show every extreme that they name: `element_slot`: in each aligned block of 512 entries (the elements of one device) every number 0 to 511 appears once.
All inputs are finite; a program needn't handle non-finite values.
Results may differ from the reference program's by a relative error of at most 0.0003.
Values sent between devices are 32-bit elements; how exact they have to be, the bound alone decides.
A program may use at most 128 MiB of HBM per device.

```python
import jax
import jax.numpy as jnp
import numpy as np
from jax import lax

ORDER = 4
ET = 1
ES = 4
EA = 128
ELEM_DEV = 512
NT = 8
NS = 16
ELEMS = 16384
N_BLK = 8
N_SPAN = 4


def draw_element_slot(key, part):
    block_keys = jax.random.split(jax.random.fold_in(key, 17), ELEMS // ELEM_DEV)

    def block_order(block_key):
        return jax.random.permutation(block_key, ELEM_DEV)
    orders = jax.vmap(block_order)(block_keys)
    return orders.reshape(ELEMS).astype(jnp.int32)


def draw_rotor_offset(key, part):
    row_keys = jax.random.split(jax.random.fold_in(key, 29), 5)
    base = jax.random.randint(row_keys[0], (NS,), 0, NT)
    far_row = N_BLK // 2 * ET + jax.random.randint(row_keys[1], (), 0, ET)
    near_row = jax.random.randint(row_keys[2], (), 1, ET + 1)
    full_row = (N_BLK - 1) * ET + jax.random.randint(row_keys[3], (), 0, ET)
    base = base.at[0].set(far_row).at[1].set(near_row).at[2].set(full_row)
    order = jax.random.permutation(row_keys[4], NS)
    return base[order].astype(jnp.int32)


def touch_ends(drawn, stream_key, low, top_value):
    spot = [jax.random.randint(jax.random.fold_in(stream_key, axis), (), 0, length) for axis, length in enumerate(drawn.shape)]
    main_axis = drawn.shape.index(max(drawn.shape))
    next_to = spot[:main_axis] + [(spot[main_axis] + 1) % drawn.shape[main_axis]] + spot[main_axis + 1:]
    return drawn.at[tuple(spot)].set(low).at[tuple(next_to)].set(top_value)


def shard_levels(key, extent, cuts, least, top_value):
    level, own = 1.0, jax.random.fold_in(key, 6)
    for position, blocks in cuts:
        steps = jnp.exp(jax.random.uniform(jax.random.fold_in(own, position), (blocks,), jnp.float32, least / len(cuts), top_value / len(cuts)))
        level = level * jnp.repeat(steps, extent[position] // blocks).reshape([-1 if axis == position else 1 for axis in range(len(extent))])
    return level


def scatter_about(own_key, dims, spread, most, cuts=(), kind=jnp.bfloat16):
    level = shard_levels(own_key, dims, cuts, -0.22, 0.18) if cuts else 1.0
    drawn = jax.random.normal(own_key, dims, jnp.float32) * spread * level
    return jnp.minimum(jnp.maximum(drawn, -most), most).astype(kind)


def setup_inputs(seed: int = 0) -> dict:
    streams_of = jax.random.split(jax.random.key(seed), 8)
    fields = scatter_about(streams_of[0], (5, (ORDER + 1) ** 3, ELEMS), 1.0, 6.0, ((2, 32),), jnp.float32)
    section_store = scatter_about(streams_of[1], (5, (ORDER + 1) ** 3, ELEMS), 1.0, 6.0, ((2, 32),), jnp.float32)
    mean_velocity = jnp.clip(jax.random.uniform(streams_of[2], (3, (ORDER + 1) ** 3, ELEMS), jnp.float32, -0.6, 0.6) * shard_levels(streams_of[2], (3, (ORDER + 1) ** 3, ELEMS), ((2, 32),), -0.4, 0.0), -0.6, 0.6)
    sound_speed = jnp.clip(0.7 + 0.8 * jax.random.uniform(streams_of[3], ((ORDER + 1) ** 3, ELEMS), jnp.float32) ** shard_levels(streams_of[3], ((ORDER + 1) ** 3, ELEMS), ((1, 32),), -0.2, 0.2), 0.7, 1.5)
    element_slot = draw_element_slot(jax.random.fold_in(streams_of[7], 71), 0)
    face_turn = touch_ends(jax.random.randint(streams_of[5], (NT, NS), 0, 8), jax.random.fold_in(streams_of[5], 1), 0, 7).astype(jnp.int32)
    rotor_offset = draw_rotor_offset(jax.random.fold_in(streams_of[7], 71), 0)
    return dict(fields=fields, section_store=section_store, mean_velocity=mean_velocity, sound_speed=sound_speed, element_slot=element_slot, face_turn=face_turn, rotor_offset=rotor_offset)


section_decay = -567301805773.0 / 1357537059087.0
section_gain = 5161836677717.0 / 13612068292357.0
time_step = 0.05
metric_scale = (1.0, 1.5, 0.75)
end_weight = 0.1

def lobatto_slopes():
    inner_root = np.sqrt(3.0 / 7.0)
    points = np.array([-1.0, -inner_root, 0.0, inner_root, 1.0])
    node_count = points.shape[0]
    slope_values = np.zeros((node_count, node_count))
    for row_index in range(node_count):
        for column_index in range(node_count):
            if row_index == column_index:
                slope_values[row_index, column_index] = sum((1.0 / (points[row_index] - points[other_index]) for other_index in range(node_count) if other_index != row_index))
            else:
                product_row = np.prod([points[row_index] - points[other_index] for other_index in range(node_count) if other_index != row_index])
                product_column = np.prod([points[column_index] - points[other_index] for other_index in range(node_count) if other_index != column_index])
                slope_values[row_index, column_index] = product_row / (product_column * (points[row_index] - points[column_index]))
    return slope_values

def face_of(element_data, direction, which_end):
    return lax.index_in_dim(element_data, which_end, axis=1 + direction, keepdims=False)

def normal_trace(face_data, direction):
    return jnp.concatenate([face_data[:5], face_data[5 + direction:6 + direction], face_data[8:9]], axis=0)

def normal_flux(face_data, direction):
    state_part = face_data[:5]
    flow_speed = face_data[5]
    sound_part = face_data[6]
    normal_velocity = state_part[1 + direction]
    pressure = state_part[4]
    zero_part = jnp.zeros_like(pressure)
    coupled = jnp.stack([normal_velocity] + [pressure if axis_index == direction else zero_part for axis_index in range(3)] + [normal_velocity])
    return flow_speed[None] * state_part + sound_part[None] * coupled

def face_flux(left_side, right_side, direction):
    wave_reach = jnp.maximum(jnp.abs(left_side[5]) + left_side[6], jnp.abs(right_side[5]) + right_side[6])
    return 0.5 * (normal_flux(left_side, direction) + normal_flux(right_side, direction)) - 0.5 * wave_reach[None] * (right_side[:5] - left_side[:5])

def wall_ghost(face_data):
    flip_sign = jnp.array([1.0, 1.0, -1.0, 1.0, 1.0, 1.0, 1.0], jnp.float32).reshape((7,) + (1,) * (face_data.ndim - 1))
    return face_data * flip_sign

def turn_face(face_data, turn_codes, inverse):
    result = jnp.zeros_like(face_data)
    for turn_code in range(8):
        turned = face_data
        if inverse:
            if turn_code & 2:
                turned = jnp.flip(turned, 2)
            if turn_code & 1:
                turned = jnp.flip(turned, 1)
            if turn_code & 4:
                turned = jnp.swapaxes(turned, 1, 2)
        else:
            if turn_code & 4:
                turned = jnp.swapaxes(turned, 1, 2)
            if turn_code & 1:
                turned = jnp.flip(turned, 1)
            if turn_code & 2:
                turned = jnp.flip(turned, 2)
        result = result + jnp.where(turn_codes == turn_code, turned, 0.0)
    return result

def pick_cells(cycle_data, cell_index):
    full_index = jnp.broadcast_to(cell_index[None, None, None], cycle_data.shape[:3] + cell_index.shape)
    return jnp.take_along_axis(cycle_data, full_index, axis=3)

def surface_terms(segment, direction, ghost_low, ghost_high):
    plus_side = normal_trace(face_of(segment, direction, 4), direction)
    minus_side = normal_trace(face_of(segment, direction, 0), direction)
    element_axis = 3 + direction
    left_side = jnp.concatenate([ghost_low, plus_side], axis=element_axis)
    right_side = jnp.concatenate([minus_side, ghost_high], axis=element_axis)
    fluxes = face_flux(left_side, right_side, direction)
    face_total = fluxes.shape[element_axis]
    upper_part = normal_flux(plus_side, direction) - lax.slice_in_dim(fluxes, 1, face_total, axis=element_axis)
    lower_part = lax.slice_in_dim(fluxes, 0, face_total - 1, axis=element_axis) - normal_flux(minus_side, direction)
    mark_shape = [1] * 7
    mark_shape[1 + direction] = 5
    high_mark = (jnp.arange(5) == 4).astype(jnp.float32).reshape(mark_shape)
    low_mark = (jnp.arange(5) == 0).astype(jnp.float32).reshape(mark_shape)
    weight = metric_scale[direction] / end_weight
    return weight * (jnp.expand_dims(upper_part, 1 + direction) * high_mark + jnp.expand_dims(lower_part, 1 + direction) * low_mark)

def volume_terms(element_data):
    slope_table = jnp.asarray(lobatto_slopes(), jnp.float32)
    einsum_forms = ('ni,fijkxyz->fnjkxyz', 'nj,fijkxyz->finkxyz', 'nk,fijkxyz->fijnxyz')
    summed = jnp.zeros((5,) + element_data.shape[1:], jnp.float32)
    for direction in range(3):
        volume_flux = normal_flux(normal_trace(element_data, direction), direction)
        summed = summed - metric_scale[direction] * jnp.einsum(einsum_forms[direction], slope_table, volume_flux, precision=lax.Precision.HIGHEST)
    return summed

def block_rates(element_data, theta_low, theta_high, span_low, span_high, from_rotor, from_stator):
    half_axial = element_data.shape[6] // 2
    rates = volume_terms(element_data)
    rates = rates + surface_terms(element_data, 0, theta_low, theta_high)
    rates = rates + surface_terms(element_data, 1, span_low, span_high)
    stator = element_data[..., :half_axial]
    rotor = element_data[..., half_axial:]
    inlet_trace = normal_trace(face_of(stator, 2, 0)[..., 0:1], 2)
    inlet = jnp.concatenate([jnp.zeros_like(inlet_trace[:5]), inlet_trace[5:]], axis=0)
    outlet_trace = normal_trace(face_of(rotor, 2, 4)[..., half_axial - 1:half_axial], 2)
    outlet = jnp.concatenate([jnp.zeros_like(outlet_trace[:5]), outlet_trace[5:]], axis=0)
    axial_terms = jnp.concatenate([surface_terms(stator, 2, inlet, from_rotor), surface_terms(rotor, 2, from_stator, outlet)], axis=6)
    return rates + axial_terms

def reference(fields, section_store, mean_velocity, sound_speed, element_slot, face_turn, rotor_offset):
    node_count = ORDER + 1
    block_count = N_BLK * N_SPAN
    half_axial = EA // 2
    cycle_size = ET * N_BLK
    block_turns = face_turn.reshape(N_BLK, ET, N_SPAN, ES)

    def block_data(block_index):
        start = block_index * ELEM_DEV
        slots = lax.dynamic_slice_in_dim(element_slot, start, ELEM_DEV, 0)
        local_fields = lax.dynamic_slice_in_dim(fields, start, ELEM_DEV, 2)
        local_velocity = lax.dynamic_slice_in_dim(mean_velocity, start, ELEM_DEV, 2)
        local_sound = lax.dynamic_slice_in_dim(sound_speed, start, ELEM_DEV, 1)
        stacked = jnp.concatenate([local_fields, local_velocity, local_sound[None]], axis=0)
        element_data = jnp.take(stacked, slots, axis=2).reshape(9, node_count, node_count, node_count, ET, ES, EA)
        return (slots, element_data)

    def codes_of(block_index):
        return block_turns[block_index // N_SPAN, :, block_index % N_SPAN, :]

    def trace_pass(block_index):
        slots, element_data = block_data(block_index)
        theta_pair = jnp.concatenate([face_of(element_data, 0, 0)[:, :, :, 0:1], face_of(element_data, 0, 4)[:, :, :, ET - 1:ET]], axis=3)
        span_pair = jnp.concatenate([face_of(element_data, 1, 0)[:, :, :, :, 0:1], face_of(element_data, 1, 4)[:, :, :, :, ES - 1:ES]], axis=4)
        stator_face = face_of(element_data, 2, 4)[..., half_axial - 1]
        rotor_face = turn_face(face_of(element_data, 2, 0)[..., half_axial], codes_of(block_index), True)
        return (theta_pair, span_pair, stator_face, rotor_face)
    block_ids = jnp.arange(block_count, dtype=jnp.int32)
    theta_pairs, span_pairs, stator_faces, rotor_faces = lax.map(trace_pass, block_ids)

    def rate_pass(block_index):
        slots, element_data = block_data(block_index)
        sector = block_index // N_SPAN
        slab_index = block_index % N_SPAN
        before = (sector - 1) % N_BLK * N_SPAN + slab_index
        after = (sector + 1) % N_BLK * N_SPAN + slab_index
        theta_low = normal_trace(theta_pairs[before][:, :, :, 1:2], 0)
        theta_high = normal_trace(theta_pairs[after][:, :, :, 0:1], 0)
        own_span = span_pairs[block_index]
        below = normal_trace(span_pairs[jnp.maximum(block_index - 1, 0)][:, :, :, :, 1:2], 1)
        above = normal_trace(span_pairs[jnp.minimum(block_index + 1, block_count - 1)][:, :, :, :, 0:1], 1)
        hub = wall_ghost(normal_trace(own_span[:, :, :, :, 0:1], 1))
        casing = wall_ghost(normal_trace(own_span[:, :, :, :, 1:2], 1))
        span_low = jnp.where(slab_index > 0, below, hub)
        span_high = jnp.where(slab_index < N_SPAN - 1, above, casing)
        cycle_blocks = jnp.arange(N_BLK, dtype=jnp.int32) * N_SPAN + slab_index
        stator_cycle = jnp.moveaxis(stator_faces[cycle_blocks], 0, 3).reshape(9, node_count, node_count, cycle_size, ES)
        rotor_cycle = jnp.moveaxis(rotor_faces[cycle_blocks], 0, 3).reshape(9, node_count, node_count, cycle_size, ES)
        cycle_cells = sector * ET + jnp.arange(ET, dtype=jnp.int32)
        offsets = lax.dynamic_slice_in_dim(rotor_offset, (slab_index * ES).astype(jnp.int32), ES, 0)
        stator_near = pick_cells(stator_cycle, (cycle_cells[:, None] - offsets[None, :]) % cycle_size)
        rotor_near = pick_cells(rotor_cycle, (cycle_cells[:, None] + offsets[None, :]) % cycle_size)
        from_stator = normal_trace(turn_face(stator_near, codes_of(block_index), False), 2)[..., None]
        from_rotor = normal_trace(rotor_near, 2)[..., None]
        rates = block_rates(element_data, theta_low, theta_high, span_low, span_high, from_rotor, from_stator)
        stored = jnp.zeros((5, node_count ** 3, ELEM_DEV), jnp.float32).at[:, :, slots].set(rates.reshape(5, node_count ** 3, ELEM_DEV))
        start = block_index * ELEM_DEV
        old_store = lax.dynamic_slice_in_dim(section_store, start, ELEM_DEV, 2)
        old_fields = lax.dynamic_slice_in_dim(fields, start, ELEM_DEV, 2)
        new_store = section_decay * old_store + time_step * stored
        new_fields = old_fields + section_gain * new_store
        return (new_fields, new_store)
    fields_blocks, store_blocks = lax.map(rate_pass, block_ids)
    fields_next = jnp.moveaxis(fields_blocks, 0, 2).reshape(5, node_count ** 3, ELEMS)
    store_next = jnp.moveaxis(store_blocks, 0, 2).reshape(5, node_count ** 3, ELEMS)
    return (fields_next, store_next)
```

```python
import functools

import jax
import jax.numpy as jnp
import numpy as np
from jax import lax
from jax.experimental import pallas as pl
from jax.experimental.pallas import tpu as pltpu
from jax.sharding import PartitionSpec as P

ORDER = 4
N1 = ORDER + 1
FACE = N1 * N1
NODES = N1**3
ROWS = 128
OFF = 32
FROWS = 32
GROUPS = ((0, 8), (8, 16), (16, 25))
SENT = ((0, 1, 2, 3, 4, 5, 8), (0, 1, 2, 3, 4, 6, 8), (0, 1, 2, 3, 4, 7, 8))

section_decay = -567301805773.0 / 1357537059087.0
section_gain = 5161836677717.0 / 13612068292357.0
time_step = 0.05
metric_scale = (1.0, 1.5, 0.75)
end_weight = 0.1
MESH = pl.DeviceIdType.MESH
F32 = jnp.float32
BF16 = jnp.bfloat16


def lobatto_slopes():
    r = np.sqrt(3.0 / 7.0)
    x = np.array([-1.0, -r, 0.0, r, 1.0])
    n = x.shape[0]
    d = np.zeros((n, n))
    for i in range(n):
        for j in range(n):
            if i == j:
                d[i, j] = sum(1.0 / (x[i] - x[m]) for m in range(n) if m != i)
            else:
                a = np.prod([x[i] - x[m] for m in range(n) if m != i])
                b = np.prod([x[j] - x[m] for m in range(n) if m != j])
                d[i, j] = a / (b * (x[i] - x[j]))
    return d


def derivative_tables():
    slopes = lobatto_slopes().astype(np.float32).astype(np.float64)
    eye = np.eye(N1)
    full = np.zeros((ROWS, 3 * ROWS))
    for d in range(3):
        mats = [eye, eye, eye]
        mats[d] = slopes
        big = np.kron(np.kron(mats[0], mats[1]), mats[2])
        full[:NODES, d * ROWS : d * ROWS + NODES] = -metric_scale[d] * big
    hi = np.asarray(full, np.float32).astype(jnp.bfloat16)
    lo = (full - hi.astype(np.float64)).astype(np.float32).astype(jnp.bfloat16)
    return np.concatenate([hi, hi], axis=1), lo


def turn_tables():
    base = np.arange(FACE).reshape(N1, N1)
    pick = np.zeros((9 * FROWS, ROWS), np.float32)
    turn = np.zeros((8 * FROWS, FROWS), np.float32)
    put = np.zeros((ROWS, 2 * FROWS), np.float32)
    for n in range(FACE):
        pick[n, N1 * n + N1 - 1] = 1
        put[N1 * n + N1 - 1, n] = 1
        put[N1 * n, FROWS + n] = 1
    for o in range(8):
        fwd = base.T if o & 4 else base
        fwd = fwd[::-1] if o & 1 else fwd
        fwd = fwd[:, ::-1] if o & 2 else fwd
        inv = base[:, ::-1] if o & 2 else base
        inv = inv[::-1] if o & 1 else inv
        inv = inv.T if o & 4 else inv
        for n in range(FACE):
            pick[(o + 1) * FROWS + n, N1 * inv.reshape(-1)[n]] = 1
            turn[o * FROWS + n, fwd.reshape(-1)[n]] = 1
    return tuple(t.astype(jnp.bfloat16) for t in (pick, turn, put))


def split(x):
    hi = x.astype(BF16)
    return hi, (x - hi.astype(F32)).astype(BF16)


def dot(a, b):
    return jnp.dot(a, b, preferred_element_type=F32)


def dot_t(a, b):
    return lax.dot_general(a, b, (((1,), (1,)), ((), ())), preferred_element_type=F32)


def flux(state, d):
    q, m, c = state[:5], state[5], state[6]
    cu, cp = c * q[1 + d], c * q[4]
    out = [m * v for v in q]
    out[0] = out[0] + cu
    out[1 + d] = out[1 + d] + cp
    out[4] = out[4] + cu
    return out


def correction(own, outer, sign, d):
    w = 0.5 * metric_scale[d] / end_weight
    reach = jnp.maximum(jnp.abs(own[5]) + own[6], jnp.abs(outer[5]) + outer[6])
    fo, fx = flux(own, d), flux(outer, d)
    return [w * (sign * (fo[k] - fx[k]) + reach * (outer[k] - own[k])) for k in range(5)]


def kernel(
    n_blk, n_span, per_span, axial, fields_in, mean_in, sound_in, slot, turns, offs, w_hi_in, w_lo_in,
    pick_in, turn_in, put_in,
    out, e, perm, fb, rates, th_send, th_recv, th_out, far_slot, cross, sp_send, sp_recv, sp_rows, pk,
    gath, own_face, slide, fields, mean, sound, w_hi, w_lo, pick, turn, put,
    th_ss, th_rs, sl_ss, sl_rs, sp_ss, sp_rs, if_ss, if_rs, loaded, ready, near,
):
    elems = per_span * axial
    half = axial // 2
    blk, slab = lax.axis_index("blk"), lax.axis_index("span")
    up, down = lax.rem(blk + 1, n_blk), lax.rem(blk + n_blk - 1, n_blk)
    right, left = lax.rem(slab + 1, n_span), lax.rem(slab + n_span - 1, n_span)

    first = pl.ds(0, 1)
    pairs = (
        (fields_in, fields), (mean_in.at[first], mean.at[first]), (sound_in, sound),
        (mean_in.at[pl.ds(1, 2)], mean.at[pl.ds(1, 2)]), (w_hi_in, w_hi), (w_lo_in, w_lo),
        (pick_in, pick), (turn_in, turn), (put_in, put),
    )
    loads = [pltpu.make_async_copy(a, b, loaded.at[n]) for n, (a, b) in enumerate(pairs)]
    for load in loads:
        load.start()
    even = lax.rem(blk, 2) == 0
    odd = jnp.logical_not(even)
    barrier = pltpu.get_barrier_semaphore()

    def greet(sem, target, cond):
        @pl.when(cond)
        def _():
            pl.semaphore_signal(sem, inc=1, device_id={"blk": target}, device_id_type=MESH)

    for k in range(1, n_blk):
        greet(barrier, lax.rem(blk + k, n_blk), blk + k < n_blk)
    greet(barrier, down, odd)
    for side in (right, left):
        pl.semaphore_signal(barrier, inc=1, device_id={"span": side}, device_id_type=MESH)

    last = NODES - FACE
    theta_own = [fields.at[k] for k in range(5)] + [mean.at[0], sound]
    for load in loads[:3]:
        load.wait()
    for a, b in GROUPS:
        for n, ref in enumerate(theta_own):
            at = 7 * a + n * (b - a)
            th_send[0, at : at + b - a] = ref[last + a : last + b]
            th_send[1, at : at + b - a] = ref[a:b]

    def remote(src, dst, ss, rs, target):
        return pltpu.make_async_remote_copy(
            src_ref=src, dst_ref=dst, send_sem=ss, recv_sem=rs, device_id=target,
            device_id_type=MESH,
        )

    def flow(side, target):
        at = [slice(7 * a, 7 * b + (b == FACE)) for a, b in GROUPS]
        return [
            remote(th_send.at[side, r], th_recv.at[side, r], th_ss.at[side, g], th_rs.at[side, g], {"blk": target})
            for g, r in enumerate(at)
        ]

    ups, dns = flow(0, up), flow(1, down)
    slots = [
        remote(slot, far_slot.at[n], sl_ss.at[n], sl_rs.at[n], {"blk": t}) for n, t in enumerate((up, down))
    ]
    pl.semaphore_wait(barrier, blk + jnp.where(even, 1, 0) + 2)
    greet(near, down, jnp.logical_and(even, blk >= 4))
    for k in range(1, n_blk):
        greet(ready, lax.rem(blk + n_blk - k, n_blk), jnp.logical_and(blk >= k, even) if k == 1 else blk >= k)

    def send(cond, copies, held=None):
        @pl.when(cond)
        def _():
            if held is not None:
                pl.semaphore_wait(held, 1)
            for copy in copies:
                copy.start()

    front = blk < 2
    rear = jnp.logical_not(front)
    send(even, [slots[0], ups[0]])
    send(odd, [slots[1], dns[0]])

    for load in loads[3:]:
        load.wait()
    cells = 2 * per_span
    lane = lax.broadcasted_iota(jnp.int32, (1, 128), 1)
    lane_f, lane_cell = lane // cells, lax.rem(lane, cells)
    lane_s = lax.rem(lane_cell, per_span)
    stator = lane_cell < per_span
    code = jnp.zeros((1, 128), jnp.int32)
    turn_by = jnp.zeros((1, 128), jnp.int32)
    for s in range(per_span):
        code = jnp.where(lane_s == s, turns[0, s], code)
        turn_by = jnp.where(lane_s == s, offs[s], turn_by)
    place = jnp.zeros((1, 128), jnp.int32)
    for c in range(cells):
        at = (c % per_span) * axial + half - 1 + c // per_span
        place = jnp.where(lane_cell == c, slot[:, at : at + 1], place)
    elem = lax.broadcasted_iota(jnp.int32, (elems, 128), 0)
    own_side = jnp.where(elem == place, 1.0, 0.0).astype(BF16)
    state = [fields.at[k] for k in range(5)] + [mean.at[d] for d in range(3)] + [sound]
    z = jnp.zeros((NODES, 128), F32)
    for n, f in enumerate(SENT[2]):
        hi, lo = split(state[f][...])
        z = jnp.where(lane_f == n, dot(hi, own_side) + dot(lo, own_side), z)
    hi, lo = split(jnp.concatenate([z, jnp.zeros((ROWS - NODES, 128), F32)], axis=0))
    picked = dot(pick[...], hi) + dot(pick[...], lo)
    own_face[...] = jnp.where(stator, picked[:FROWS], picked[FROWS : 2 * FROWS])
    packet = picked[:FROWS]
    for o in range(8):
        part = picked[(o + 1) * FROWS : (o + 2) * FROWS]
        packet = jnp.where(jnp.logical_and(jnp.logical_not(stator), code == o), part, packet)
    half_rows = FROWS // 2
    pk[...] = jnp.where(lane < 64, packet[:half_rows], pltpu.roll(packet[half_rows:], 64, 1))
    if_copies = [
        remote(pk, gath.at[k - 1], if_ss.at[k - 1], if_rs.at[k - 1], {"blk": lax.rem(blk + k, n_blk)})
        for k in range(1, n_blk)
    ]
    for k, copy in enumerate(if_copies, 1):
        send(blk + k >= n_blk, [copy])
    send(jnp.logical_and(even, front), [ups[1]])
    send(jnp.logical_and(odd, front), [dns[1]])
    send(jnp.logical_and(even, rear), [slots[1], dns[0]])
    send(jnp.logical_and(jnp.logical_and(odd, rear), blk < n_blk - 1), [slots[0], ups[0]], near)
    send(blk == n_blk - 1, [slots[0], ups[0]])

    rows_i = lax.broadcasted_iota(jnp.int32, (elems, elems), 0)
    perm[...] = jnp.where(rows_i == slot[...], 1.0, 0.0).astype(BF16)

    def gather(f, value):
        hi, lo = split(value)
        e[f, :OFF] = jnp.zeros((OFF, elems), F32)
        e[f, OFF + 120 :] = jnp.zeros((e.shape[1] - OFF - 120, elems), F32)
        e[f, OFF : OFF + NODES] = dot(hi, perm[...]) + dot(lo, perm[...])

    for f in range(9):
        gather(f, state[f][...])

    block = slice(OFF, OFF + ROWS)
    for n, f in enumerate(SENT[1]):
        for i in range(N1):
            at = OFF + i * FACE
            sp_send[0, n, i * N1 : (i + 1) * N1] = e[f, at + 20 : at + 25, elems - axial :]
            sp_send[1, n, i * N1 : (i + 1) * N1] = e[f, at : at + 5, :axial]
    sp_up = remote(sp_send.at[0], sp_recv.at[0], sp_ss.at[0], sp_rs.at[0], {"span": right})
    sp_dn = remote(sp_send.at[1], sp_recv.at[1], sp_ss.at[1], sp_rs.at[1], {"span": left})
    inner_hi, inner_lo = slab < n_span - 1, slab > 0
    send(inner_hi, [sp_up])
    send(inner_lo, [sp_dn])
    for s in range(per_span):
        ln = slice(s * axial, (s + 1) * axial)
        for d in range(3):
            for k, v in enumerate(flux([e[f, block, ln] for f in SENT[d]], d)):
                hi, lo = split(v)
                at = slice(k * elems + s * axial, k * elems + (s + 1) * axial)
                fb[d * ROWS : (d + 1) * ROWS, at] = hi
                fb[(3 + d) * ROWS : (4 + d) * ROWS, at] = lo
    for k in range(5):
        at = slice(k * elems, (k + 1) * elems)
        rates[k] = dot(w_hi[...], fb[:, at]) + dot(w_lo[...], fb[: 3 * ROWS, at])

    above = n_blk - 1 - blk - jnp.where(even, 1, 0)

    @pl.when(above > 0)
    def _():
        pl.semaphore_wait(ready, above)

    for k, copy in enumerate(if_copies, 1):
        send(blk + k < n_blk, [copy])
    send(jnp.logical_and(even, front), [ups[2], slots[1], *dns])
    send(jnp.logical_and(odd, front), [dns[2], slots[0], *ups])
    send(jnp.logical_and(even, rear), [*dns[1:], *ups[1:]])
    send(jnp.logical_and(odd, rear), [*ups[1:], *dns[1:]])

    for side, copy in enumerate(slots):
        copy.wait()
        far = jnp.where(rows_i == far_slot[side], 1.0, 0.0).astype(BF16)
        cross[side] = dot_t(far, perm[...]).astype(BF16)

    row = lax.broadcasted_iota(jnp.int32, (ROWS, axial), 0)
    a_id = lax.broadcasted_iota(jnp.int32, (ROWS, axial), 1)
    k_id = lax.rem(row // N1, N1)

    @pl.when(inner_hi)
    def _():
        sp_up.wait_send()
        sp_dn.wait_recv()

    @pl.when(inner_lo)
    def _():
        sp_dn.wait_send()
        sp_up.wait_recv()

    for n in range(7):
        for i in range(N1):
            at = i * FACE
            sp_rows[n, at : at + 5] = sp_recv[0, n, i * N1 : (i + 1) * N1]
            sp_rows[n, at + 20 : at + 25] = sp_recv[1, n, i * N1 : (i + 1) * N1]
    low = k_id == 0
    face = jnp.logical_and(jnp.logical_or(low, k_id == N1 - 1), row < NODES)
    sign = jnp.where(low, -1.0, 1.0)
    for s in range(per_span):
        ln = slice(s * axial, (s + 1) * axial)
        own = [e[f, block, ln] for f in SENT[1]]
        outer = []
        for n, f in enumerate(SENT[1]):
            wall = -own[n] if n == 2 else own[n]
            if s == 0:
                lo_v = jnp.where(slab > 0, sp_rows[n], wall)
            else:
                lo_v = e[f, OFF + 20 : OFF + 20 + ROWS, (s - 1) * axial : s * axial]
            if s == per_span - 1:
                hi_v = jnp.where(slab < n_span - 1, sp_rows[n], wall)
            else:
                hi_v = e[f, OFF - 20 : OFF - 20 + ROWS, (s + 1) * axial : (s + 2) * axial]
            outer.append(jnp.where(low, lo_v, hi_v))
        for k, v in enumerate(correction(own, outer, sign, 1)):
            rates[k, :, ln] += jnp.where(face, v, 0.0)

    l_id = lax.rem(row, N1)
    low = l_id == 0
    face = jnp.logical_and(jnp.logical_or(low, l_id == N1 - 1), row < NODES)
    sign = jnp.where(low, -1.0, 1.0)
    slides = a_id == jnp.where(low, half, half - 1)
    ends = a_id == jnp.where(low, 0, axial - 1)
    for s in range(per_span):
        ln = slice(s * axial, (s + 1) * axial)
        own = [e[f, block, ln] for f in SENT[2]]
        outer = []
        for n, f in enumerate(SENT[2]):
            lo_v = pltpu.roll(e[f, OFF + 4 : OFF + 4 + ROWS, ln], 1, 1)
            hi_v = pltpu.roll(e[f, OFF - 4 : OFF - 4 + ROWS, ln], axial - 1, 1)
            v = jnp.where(slides, own[n], jnp.where(low, lo_v, hi_v))
            outer.append(jnp.where(ends, own[n] if n > 4 else 0.0, v))
        for k, v in enumerate(correction(own, outer, sign, 2)):
            rates[k, :, ln] += jnp.where(face, v, 0.0)

    for k in range(5):
        hi, lo = split(rates[k])
        out[k] = (dot_t(hi, perm[...]) + dot_t(lo, perm[...]))[:NODES]

    for copy in if_copies:
        copy.wait()
    steps = jnp.where(stator, turn_by, lax.rem(n_blk - turn_by, n_blk))
    chosen = pk[...]
    for k in range(1, n_blk):
        chosen = jnp.where(steps == k, gath[k - 1], chosen)
    chosen = jnp.concatenate([chosen, pltpu.roll(chosen, 64, 1)], axis=0)
    hi, lo = split(chosen)
    parts = dot(turn[...], hi) + dot(turn[...], lo)
    for o in range(8):
        chosen = jnp.where(jnp.logical_and(stator, code == o), parts[o * FROWS : (o + 1) * FROWS], chosen)
    outer = jnp.where(stator, pltpu.roll(chosen, 128 - per_span, 1), pltpu.roll(chosen, per_span, 1))

    def traces(x):
        return [x if n == 0 else pltpu.roll(x, 128 - n * cells, 1) for n in range(7)]

    sgn = jnp.where(stator, 1.0, -1.0)
    for k, v in enumerate(correction(traces(own_face[...]), traces(outer), sgn, 2)):
        at = slice(k * 128, (k + 1) * 128)
        slide[:FROWS, at] = jnp.where(lane < per_span, v, 0.0)
        slide[FROWS:, at] = jnp.where(jnp.logical_and(lane >= per_span, lane < cells), v, 0.0)
    hi, lo = split(slide[...])
    jumps = dot(put[...], hi) + dot(put[...], lo)
    for k in range(5):
        hi, lo = split(jumps[:, k * 128 : (k + 1) * 128])
        out[k] += (dot_t(hi, own_side) + dot_t(lo, own_side))[:NODES]

    def theta(side, first, sgn, copies):
        for (a, b), copy in zip(GROUPS, copies):
            copy.wait()
            rows = slice(7 * a, 7 * b)
            hi, lo = split(th_recv[side, rows])
            th_out[rows] = dot(hi, cross[side]) + dot(lo, cross[side])
            own = [ref[first + a : first + b] for ref in theta_own]
            outer = [th_out[7 * a + n * (b - a) : 7 * a + (n + 1) * (b - a)] for n in range(7)]
            for k, v in enumerate(correction(own, outer, sgn, 0)):
                out[k, first + a : first + b] += v

    @pl.when(even)
    def _():
        theta(0, 0, -1.0, ups)
        theta(1, last, 1.0, dns)

    @pl.when(odd)
    def _():
        theta(1, last, 1.0, dns)
        theta(0, 0, -1.0, ups)


def on_device(fields, store, mean, sound, slot, turns, offs, n_blk, n_span):
    per_theta, per_span = turns.shape
    assert per_theta == 1 and n_blk % 2 == 0
    elems = slot.shape[0]
    axial = elems // per_span
    w_hi, w_lo = (jnp.asarray(t) for t in derivative_tables())
    pick, turn, put = (jnp.asarray(t) for t in turn_tables())
    vmem = pl.BlockSpec(memory_space=pltpu.VMEM)
    hbm = pl.BlockSpec(memory_space=pl.ANY)
    smem = pl.BlockSpec(memory_space=pltpu.SMEM)
    dma = pltpu.SemaphoreType.DMA
    stored = pl.pallas_call(
        functools.partial(kernel, n_blk, n_span, per_span, axial),
        out_shape=jax.ShapeDtypeStruct((5, NODES, elems), F32),
        in_specs=[hbm] * 3 + [vmem] + [smem] * 2 + [hbm] * 5,
        out_specs=vmem,
        scratch_shapes=[
            pltpu.VMEM((9, OFF + ROWS + 32, elems), F32),
            pltpu.VMEM((elems, elems), BF16),
            pltpu.VMEM((6 * ROWS, 5 * elems), BF16),
            pltpu.VMEM((5, ROWS, elems), F32),
            pltpu.VMEM((2, 7 * FACE + 1, elems), F32),
            pltpu.VMEM((2, 7 * FACE + 1, elems), F32),
            pltpu.VMEM((7 * FACE + 1, elems), F32),
            pltpu.VMEM((2, 1, elems), jnp.int32),
            pltpu.VMEM((2, elems, elems), BF16),
            pltpu.VMEM((2, 7, FROWS, axial), F32),
            pltpu.VMEM((2, 7, FROWS, axial), F32),
            pltpu.VMEM((7, ROWS, axial), F32),
            pltpu.VMEM((FROWS // 2, 128), F32),
            pltpu.VMEM((n_blk - 1, FROWS // 2, 128), F32),
            pltpu.VMEM((FROWS, 128), F32),
            pltpu.VMEM((2 * FROWS, 5 * 128), F32),
            pltpu.VMEM(fields.shape, F32),
            pltpu.VMEM(mean.shape, F32),
            pltpu.VMEM(sound.shape, F32),
            *(pltpu.VMEM(t.shape, BF16) for t in (w_hi, w_lo, pick, turn, put)),
            dma((2, len(GROUPS))), dma((2, len(GROUPS))), dma((2,)), dma((2,)), dma((2,)), dma((2,)),
            dma((n_blk - 1,)), dma((n_blk - 1,)), dma((9,)),
            pltpu.SemaphoreType.REGULAR, pltpu.SemaphoreType.REGULAR,
        ],
        compiler_params=pltpu.CompilerParams(collective_id=0, has_side_effects=True),
    )(fields, mean, sound, slot.reshape(1, elems), turns, offs, w_hi, w_lo, pick, turn, put)
    store_next = section_decay * store + time_step * stored
    return fields + section_gain * store_next, store_next


def solution(mesh):
    whole = P(None, None, ("blk", "span"))
    in_specs = (
        whole, whole, whole, P(None, ("blk", "span")), P(("blk", "span")), P("blk", "span"), P("span"),
    )
    body = functools.partial(on_device, n_blk=mesh.shape["blk"], n_span=mesh.shape["span"])
    return jax.shard_map(
        body, mesh=mesh, in_specs=in_specs, out_specs=(whole, whole), check_vma=False
    )
```

```python
import functools

import jax
import jax.numpy as jnp
import numpy as np
from jax import lax
from jax.experimental import pallas as pl
from jax.experimental.pallas import tpu as pltpu
from jax.sharding import PartitionSpec as P

ORDER = 4
N1 = ORDER + 1
FACE = N1 * N1
NODES = N1**3
ROWS = 128
OFF = 32
FROWS = 32
GROUPS = ((0, 9), (9, 17), (17, 25))
FIRST = GROUPS[0][1]
REST = FACE - FIRST
SENT = ((0, 1, 2, 3, 4, 5, 8), (0, 1, 2, 3, 4, 6, 8), (0, 1, 2, 3, 4, 7, 8))

section_decay = -567301805773.0 / 1357537059087.0
section_gain = 5161836677717.0 / 13612068292357.0
time_step = 0.05
metric_scale = (1.0, 1.5, 0.75)
end_weight = 0.1
MESH = pl.DeviceIdType.MESH
F32 = jnp.float32
BF16 = jnp.bfloat16


def lobatto_slopes():
    r = np.sqrt(3.0 / 7.0)
    x = np.array([-1.0, -r, 0.0, r, 1.0])
    n = x.shape[0]
    d = np.zeros((n, n))
    for i in range(n):
        for j in range(n):
            if i == j:
                d[i, j] = sum(1.0 / (x[i] - x[m]) for m in range(n) if m != i)
            else:
                a = np.prod([x[i] - x[m] for m in range(n) if m != i])
                b = np.prod([x[j] - x[m] for m in range(n) if m != j])
                d[i, j] = a / (b * (x[i] - x[j]))
    return d


def derivative_tables():
    slopes = lobatto_slopes().astype(np.float32).astype(np.float64)
    eye = np.eye(N1)
    full = np.zeros((ROWS, 3 * ROWS))
    for d in range(3):
        mats = [eye, eye, eye]
        mats[d] = slopes
        big = np.kron(np.kron(mats[0], mats[1]), mats[2])
        full[:NODES, d * ROWS : d * ROWS + NODES] = -metric_scale[d] * big
    hi = np.asarray(full, np.float32).astype(jnp.bfloat16)
    lo = (full - hi.astype(np.float64)).astype(np.float32).astype(jnp.bfloat16)
    return np.concatenate([hi, hi], axis=1), lo


def turn_tables():
    base = np.arange(FACE).reshape(N1, N1)
    pick = np.zeros((9 * FROWS, ROWS), np.float32)
    turn = np.zeros((8 * FROWS, FROWS), np.float32)
    put = np.zeros((ROWS, 2 * FROWS), np.float32)
    for n in range(FACE):
        pick[n, N1 * n + N1 - 1] = 1
        put[N1 * n + N1 - 1, n] = 1
        put[N1 * n, FROWS + n] = 1
    for o in range(8):
        fwd = base.T if o & 4 else base
        fwd = fwd[::-1] if o & 1 else fwd
        fwd = fwd[:, ::-1] if o & 2 else fwd
        inv = base[:, ::-1] if o & 2 else base
        inv = inv[::-1] if o & 1 else inv
        inv = inv.T if o & 4 else inv
        for n in range(FACE):
            pick[(o + 1) * FROWS + n, N1 * inv.reshape(-1)[n]] = 1
            turn[o * FROWS + n, fwd.reshape(-1)[n]] = 1
    return tuple(t.astype(jnp.bfloat16) for t in (pick, turn, put))


def split(x):
    hi = x.astype(BF16)
    return hi, (x - hi.astype(F32)).astype(BF16)


def dot(a, b):
    return jnp.dot(a, b, preferred_element_type=F32)


def dot_t(a, b):
    return lax.dot_general(a, b, (((1,), (1,)), ((), ())), preferred_element_type=F32)


def flux(state, d):
    q, m, c = state[:5], state[5], state[6]
    cu, cp = c * q[1 + d], c * q[4]
    out = [m * v for v in q]
    out[0] = out[0] + cu
    out[1 + d] = out[1 + d] + cp
    out[4] = out[4] + cu
    return out


def correction(own, outer, sign, d):
    w = 0.5 * metric_scale[d] / end_weight
    reach = jnp.maximum(jnp.abs(own[5]) + own[6], jnp.abs(outer[5]) + outer[6])
    fo, fx = flux(own, d), flux(outer, d)
    return [w * (sign * (fo[k] - fx[k]) + reach * (outer[k] - own[k])) for k in range(5)]


def merge(q, m, c, reach, d):
    return [f + reach * v for f, v in zip(flux([*q, m, c], d), q)]


def kernel(
    n_blk, n_span, per_span, axial, fields_in, mean_in, sound_in, slot, turns, offs, w_hi_in, w_lo_in,
    pick_in, turn_in, put_in,
    out_hbm, out, e, perm, fb, rates, th_send, th_recv, th_out, rate_send, rate_recv, up_send, up_recv, up_own, fix, far_slot, cross, sp_send, sp_recv, sp_rows, pk,
    gath, own_face, slide, fields, mean, sound, w_hi, w_lo, pick, turn, put,
    th_ss, th_rs, ra_ss, ra_rs, up_ss, up_rs, sl_ss, sl_rs, sp_ss, sp_rs, if_ss, if_rs, loaded, saved, ready, near,
):
    elems = per_span * axial
    half = axial // 2
    blk, slab = lax.axis_index("blk"), lax.axis_index("span")
    up, down = lax.rem(blk + 1, n_blk), lax.rem(blk + n_blk - 1, n_blk)
    right, left = lax.rem(slab + 1, n_span), lax.rem(slab + n_span - 1, n_span)

    first = pl.ds(0, 1)
    pairs = (
        (mean_in.at[first], mean.at[first]), (sound_in, sound), (fields_in, fields),
        (mean_in.at[pl.ds(1, 2)], mean.at[pl.ds(1, 2)]), (w_hi_in, w_hi), (w_lo_in, w_lo),
        (pick_in, pick), (turn_in, turn), (put_in, put),
    )
    loads = [pltpu.make_async_copy(a, b, loaded.at[n]) for n, (a, b) in enumerate(pairs)]
    for load in loads:
        load.start()
    even = lax.rem(blk, 2) == 0
    odd = jnp.logical_not(even)
    barrier = pltpu.get_barrier_semaphore()

    def greet(sem, target, cond):
        @pl.when(cond)
        def _():
            pl.semaphore_signal(sem, inc=1, device_id={"blk": target}, device_id_type=MESH)

    for k in range(1, n_blk):
        greet(barrier, lax.rem(blk + k, n_blk), blk + k < n_blk)
    greet(barrier, down, odd)
    for side in (right, left):
        pl.semaphore_signal(barrier, inc=1, device_id={"span": side}, device_id_type=MESH)

    last = NODES - FACE
    theta_own = [fields.at[k] for k in range(5)] + [mean.at[0], sound]
    near_side = lax.rem(blk, 2)
    far_side = 1 - near_side
    near_blk = jnp.where(even, up, down)
    far_blk = jnp.where(even, down, up)
    tail = blk == n_blk - 1
    wrap = jnp.logical_or(blk == 0, tail)
    inner = jnp.logical_not(wrap)

    def remote(src, dst, ss, rs, target):
        return pltpu.make_async_remote_copy(
            src_ref=src, dst_ref=dst, send_sem=ss, recv_sem=rs, device_id=target,
            device_id_type=MESH,
        )

    def flow(side, target):
        to = {"blk": target}
        slot_copy = remote(slot, far_slot.at[side], sl_ss.at[side], sl_rs.at[side], to)
        rate = remote(rate_send.at[side], rate_recv.at[side], ra_ss.at[side], ra_rs.at[side], to)
        full = []
        for g, (a, b) in enumerate(GROUPS):
            r = slice(7 * a + (g > 0), 7 * b + 1)
            full.append(remote(th_send.at[side, r], th_recv.at[side, r], th_ss.at[side, g], th_rs.at[side, g], to))
        half_size = 5 * REST // 2
        part = []
        for g in range(2):
            r = slice(g * half_size, (g + 1) * half_size)
            part.append(remote(up_send.at[side, r], up_recv.at[side, r], up_ss.at[side, g], up_rs.at[side, g], to))
        return slot_copy, rate, full, part

    def send(cond, copies, held=None):
        @pl.when(cond)
        def _():
            if held is not None:
                pl.semaphore_wait(held, 1)
            for copy in copies:
                copy.start()

    pl.semaphore_wait(barrier, blk + jnp.where(even, 1, 0) + 2)
    greet(near, down, jnp.logical_and(even, blk > 0))
    for k in range(1, n_blk):
        greet(ready, lax.rem(blk + n_blk - k, n_blk), jnp.logical_and(blk >= k, even) if k == 1 else blk >= k)
    near_slot, near_rate, near_full, near_part = flow(near_side, near_blk)
    far_slot_copy, far_rate, far_full, far_part = flow(far_side, far_blk)
    for load in loads[:2]:
        load.wait()
    for side, at in enumerate((last, 0)):
        rows = slice(at + FIRST, at + FACE)
        rate_send[side] = jnp.abs(mean[0, rows]) + sound[rows]
    near_slot.start()
    near_rate.start()
    send(jnp.logical_and(even, inner), [far_slot_copy, far_rate])
    loads[2].wait()
    for g, (a, b) in enumerate(GROUPS):
        for n, ref in enumerate(theta_own):
            at = 7 * a + (g > 0) + n * (b - a)
            th_send[0, at : at + b - a] = ref[last + a : last + b]
            th_send[1, at : at + b - a] = ref[a:b]
    send(tail, [far_slot_copy, *far_full])
    near_full[0].start()
    send(jnp.logical_and(even, inner), [far_full[0]])

    rows_i = lax.broadcasted_iota(jnp.int32, (elems, elems), 0)
    perm[...] = jnp.where(rows_i == slot[...], 1.0, 0.0).astype(BF16)


    def link(side):
        hi, lo = split(jnp.broadcast_to(far_slot[side].astype(F32), (8, elems)))
        source = (dot_t(hi, perm[...]) + dot_t(lo, perm[...]))[:1].astype(jnp.int32)
        cross[side] = jnp.where(rows_i == source, 1.0, 0.0).astype(BF16)

    def blend(side):
        sgn = jnp.where(side == 0, 1.0, -1.0)
        hi, lo = split(rate_recv[1 - side])
        there = dot(hi, cross[1 - side]) + dot(lo, cross[1 - side])
        reach = sgn * jnp.maximum(rate_send[side], there)
        for g, (a, b) in enumerate(GROUPS[1:]):
            at = 7 * a + 1
            own = [th_send[side, at + n * (b - a) : at + (n + 1) * (b - a)] for n in range(7)]
            speed = reach[a - FIRST : b - FIRST]
            for sign, ref in ((1.0, up_send), (-1.0, up_own)):
                for k, v in enumerate(merge(own[:5], own[5], own[6], sign * speed, 0)):
                    to = 5 * (a - FIRST) + k * (b - a)
                    ref[side, to : to + b - a] = v

    in_near = flow(far_side, near_blk)
    in_far = flow(near_side, far_blk)
    def settle_near():
        in_near[0].wait_recv()
        link(far_side)
        in_near[1].wait_recv()
        blend(near_side)
        near_part[0].start()
        near_part[1].start()


    for load in loads[3:]:
        load.wait()
    cells = 2 * per_span
    lane = lax.broadcasted_iota(jnp.int32, (1, 128), 1)
    lane_f, lane_cell = lane // cells, lax.rem(lane, cells)
    lane_s = lax.rem(lane_cell, per_span)
    stator = lane_cell < per_span
    code = jnp.zeros((1, 128), jnp.int32)
    turn_by = jnp.zeros((1, 128), jnp.int32)
    for s in range(per_span):
        code = jnp.where(lane_s == s, turns[0, s], code)
        turn_by = jnp.where(lane_s == s, offs[s], turn_by)
    place = jnp.zeros((1, 128), jnp.int32)
    for c in range(cells):
        at = (c % per_span) * axial + half - 1 + c // per_span
        place = jnp.where(lane_cell == c, slot[:, at : at + 1], place)
    elem = lax.broadcasted_iota(jnp.int32, (elems, 128), 0)
    own_side = jnp.where(elem == place, 1.0, 0.0).astype(BF16)
    state = [fields.at[k] for k in range(5)] + [mean.at[d] for d in range(3)] + [sound]
    z = jnp.zeros((NODES, 128), F32)
    for n, f in enumerate(SENT[2]):
        hi, lo = split(state[f][...])
        z = jnp.where(lane_f == n, dot(hi, own_side) + dot(lo, own_side), z)
    hi, lo = split(jnp.concatenate([z, jnp.zeros((ROWS - NODES, 128), F32)], axis=0))
    picked = dot(pick[...], hi) + dot(pick[...], lo)
    own_face[...] = jnp.where(stator, picked[:FROWS], picked[FROWS : 2 * FROWS])
    packet = picked[:FROWS]
    for o in range(8):
        part = picked[(o + 1) * FROWS : (o + 2) * FROWS]
        packet = jnp.where(jnp.logical_and(jnp.logical_not(stator), code == o), part, packet)
    half_rows = FROWS // 2
    pk[...] = jnp.where(lane < 64, packet[:half_rows], pltpu.roll(packet[half_rows:], 64, 1))
    if_copies = [
        remote(pk, gath.at[k - 1], if_ss.at[k - 1], if_rs.at[k - 1], {"blk": lax.rem(blk + k, n_blk)})
        for k in range(1, n_blk)
    ]
    for k, copy in enumerate(if_copies, 1):
        send(blk + k >= n_blk, [copy])
    send(jnp.logical_and(odd, inner), [far_slot_copy, far_rate, far_full[0]], near)

    def gather(f, value):
        hi, lo = split(value)
        e[f, :OFF] = jnp.zeros((OFF, elems), F32)
        e[f, OFF + 120 :] = jnp.zeros((e.shape[1] - OFF - 120, elems), F32)
        e[f, OFF : OFF + NODES] = dot(hi, perm[...]) + dot(lo, perm[...])

    for f in range(9):
        gather(f, state[f][...])

    block = slice(OFF, OFF + ROWS)
    for n, f in enumerate(SENT[1]):
        for i in range(N1):
            at = OFF + i * FACE
            sp_send[0, n, i * N1 : (i + 1) * N1] = e[f, at + 20 : at + 25, elems - axial :]
            sp_send[1, n, i * N1 : (i + 1) * N1] = e[f, at : at + 5, :axial]
    sp_up = remote(sp_send.at[0], sp_recv.at[0], sp_ss.at[0], sp_rs.at[0], {"span": right})
    sp_dn = remote(sp_send.at[1], sp_recv.at[1], sp_ss.at[1], sp_rs.at[1], {"span": left})
    inner_hi, inner_lo = slab < n_span - 1, slab > 0
    send(inner_hi, [sp_up])
    send(inner_lo, [sp_dn])

    above = n_blk - 1 - blk - jnp.where(even, 1, 0)

    @pl.when(above > 0)
    def _():
        pl.semaphore_wait(ready, above)

    for k, copy in enumerate(if_copies, 1):
        send(blk + k < n_blk, [copy])
    send(blk == 0, [far_slot_copy, *far_full])
    settle_near()
    @pl.when(inner)
    def _():
        in_far[0].wait_recv()
        link(near_side)
        in_far[1].wait_recv()
        blend(far_side)
        far_part[0].start()
        far_part[1].start()

    for s in range(per_span):
        ln = slice(s * axial, (s + 1) * axial)
        for d in range(3):
            for k, v in enumerate(flux([e[f, block, ln] for f in SENT[d]], d)):
                hi, lo = split(v)
                at = slice(k * elems + s * axial, k * elems + (s + 1) * axial)
                fb[d * ROWS : (d + 1) * ROWS, at] = hi
                fb[(3 + d) * ROWS : (4 + d) * ROWS, at] = lo
    for k in range(5):
        at = slice(k * elems, (k + 1) * elems)
        rates[k] = dot(w_hi[...], fb[:, at]) + dot(w_lo[...], fb[: 3 * ROWS, at])


    row = lax.broadcasted_iota(jnp.int32, (ROWS, axial), 0)
    a_id = lax.broadcasted_iota(jnp.int32, (ROWS, axial), 1)
    k_id = lax.rem(row // N1, N1)

    @pl.when(inner_hi)
    def _():
        sp_up.wait_send()
        sp_dn.wait_recv()

    @pl.when(inner_lo)
    def _():
        sp_dn.wait_send()
        sp_up.wait_recv()

    for n in range(7):
        for i in range(N1):
            at = i * FACE
            sp_rows[n, at : at + 5] = sp_recv[0, n, i * N1 : (i + 1) * N1]
            sp_rows[n, at + 20 : at + 25] = sp_recv[1, n, i * N1 : (i + 1) * N1]
    low = k_id == 0
    face = jnp.logical_and(jnp.logical_or(low, k_id == N1 - 1), row < NODES)
    sign = jnp.where(low, -1.0, 1.0)
    for s in range(per_span):
        ln = slice(s * axial, (s + 1) * axial)
        own = [e[f, block, ln] for f in SENT[1]]
        outer = []
        for n, f in enumerate(SENT[1]):
            wall = -own[n] if n == 2 else own[n]
            if s == 0:
                lo_v = jnp.where(slab > 0, sp_rows[n], wall)
            else:
                lo_v = e[f, OFF + 20 : OFF + 20 + ROWS, (s - 1) * axial : s * axial]
            if s == per_span - 1:
                hi_v = jnp.where(slab < n_span - 1, sp_rows[n], wall)
            else:
                hi_v = e[f, OFF - 20 : OFF - 20 + ROWS, (s + 1) * axial : (s + 2) * axial]
            outer.append(jnp.where(low, lo_v, hi_v))
        for k, v in enumerate(correction(own, outer, sign, 1)):
            rates[k, :, ln] += jnp.where(face, v, 0.0)

    l_id = lax.rem(row, N1)
    low = l_id == 0
    face = jnp.logical_and(jnp.logical_or(low, l_id == N1 - 1), row < NODES)
    sign = jnp.where(low, -1.0, 1.0)
    slides = a_id == jnp.where(low, half, half - 1)
    ends = a_id == jnp.where(low, 0, axial - 1)
    for s in range(per_span):
        ln = slice(s * axial, (s + 1) * axial)
        own = [e[f, block, ln] for f in SENT[2]]
        outer = []
        for n, f in enumerate(SENT[2]):
            lo_v = pltpu.roll(e[f, OFF + 4 : OFF + 4 + ROWS, ln], 1, 1)
            hi_v = pltpu.roll(e[f, OFF - 4 : OFF - 4 + ROWS, ln], axial - 1, 1)
            v = jnp.where(slides, own[n], jnp.where(low, lo_v, hi_v))
            outer.append(jnp.where(ends, own[n] if n > 4 else 0.0, v))
        for k, v in enumerate(correction(own, outer, sign, 2)):
            rates[k, :, ln] += jnp.where(face, v, 0.0)

    for k in range(5):
        hi, lo = split(rates[k])
        out[k] = (dot_t(hi, perm[...]) + dot_t(lo, perm[...]))[:NODES]

    @pl.when(wrap)
    def _():
        in_far[0].wait_recv()
        link(near_side)

    for copy in if_copies:
        copy.wait()
    steps = jnp.where(stator, turn_by, lax.rem(n_blk - turn_by, n_blk))
    chosen = pk[...]
    for k in range(1, n_blk):
        chosen = jnp.where(steps == k, gath[k - 1], chosen)
    chosen = jnp.concatenate([chosen, pltpu.roll(chosen, 64, 1)], axis=0)
    hi, lo = split(chosen)
    parts = dot(turn[...], hi) + dot(turn[...], lo)
    for o in range(8):
        chosen = jnp.where(jnp.logical_and(stator, code == o), parts[o * FROWS : (o + 1) * FROWS], chosen)
    outer = jnp.where(stator, pltpu.roll(chosen, 128 - per_span, 1), pltpu.roll(chosen, per_span, 1))

    def traces(x):
        return [x if n == 0 else pltpu.roll(x, 128 - n * cells, 1) for n in range(7)]

    sgn = jnp.where(stator, 1.0, -1.0)
    for k, v in enumerate(correction(traces(own_face[...]), traces(outer), sgn, 2)):
        at = slice(k * 128, (k + 1) * 128)
        slide[:FROWS, at] = jnp.where(lane < per_span, v, 0.0)
        slide[FROWS:, at] = jnp.where(jnp.logical_and(lane >= per_span, lane < cells), v, 0.0)
    hi, lo = split(slide[...])
    jumps = dot(put[...], hi) + dot(put[...], lo)
    for k in range(5):
        hi, lo = split(jumps[:, k * 128 : (k + 1) * 128])
        out[k] += (dot_t(hi, own_side) + dot_t(lo, own_side))[:NODES]

    mid = pltpu.make_async_copy(out.at[:, 32:96], out_hbm.at[:5, 32:96], saved.at[0])
    mid.start()

    def add(side, a, b):
        for at, cond in ((0, side == 0), (last, side == 1)):
            @pl.when(cond)
            def _():
                for k in range(5):
                    out[k, at + a : at + b] += fix[k, : b - a]

    def theta(side, g, copy):
        copy.wait_recv()
        a, b = GROUPS[g]
        at = 7 * a + (g > 0)
        hi, lo = split(th_recv[side, at : at + 7 * (b - a)])
        th_out[: 7 * (b - a)] = dot(hi, cross[side]) + dot(lo, cross[side])
        own = [th_send[1 - side, at + n * (b - a) : at + (n + 1) * (b - a)] for n in range(7)]
        outer = [th_out[n * (b - a) : (n + 1) * (b - a)] for n in range(7)]
        sgn = jnp.where(side == 0, -1.0, 1.0)
        for k, v in enumerate(correction(own, outer, sgn, 0)):
            fix[k, : b - a] = v
        add(side, a, b)

    def blended(side, g, copy):
        copy.wait_recv()
        a, b = GROUPS[g]
        at = 5 * (a - FIRST)
        hi, lo = split(up_recv[side, at : at + 5 * (b - a)])
        there = dot(hi, cross[side]) + dot(lo, cross[side])
        w = 0.5 * metric_scale[0] / end_weight * jnp.where(side == 0, -1.0, 1.0)
        for k in range(5):
            n = slice(k * (b - a), (k + 1) * (b - a))
            fix[k, : b - a] = w * (up_own[1 - side, at + k * (b - a) : at + (k + 1) * (b - a)] - there[n])
        add(side, a, b)

    theta(far_side, 0, in_near[2][0])
    theta(near_side, 0, in_far[2][0])

    @pl.when(wrap)
    def _():
        for g in (1, 2):
            blended(far_side, g, in_near[3][g - 1])
        for g in (1, 2):
            theta(near_side, g, in_far[2][g])
            far_full[g].wait_send()

    @pl.when(inner)
    def _():
        blended(far_side, 1, in_near[3][0])
        for g in (1, 2):
            blended(near_side, g, in_far[3][g - 1])
            far_part[g - 1].wait_send()
        blended(far_side, 2, in_near[3][1])
        far_rate.wait_send()

    lows = pltpu.make_async_copy(out.at[:, :32], out_hbm.at[:5, :32], saved.at[1])
    highs = pltpu.make_async_copy(out.at[:, 96:], out_hbm.at[:5, 96:], saved.at[2])
    lows.start()
    highs.start()
    for copy in (near_slot, near_rate, near_full[0], *near_part, far_slot_copy, far_full[0]):
        copy.wait_send()
    for copy in (mid, lows, highs):
        copy.wait()


def finish(stored_in, fields, store, fields_out, store_out, stored, fields_next, store_next, in_sem, f_sem, s_sem):
    count = stored.shape[0]
    loads = [pltpu.make_async_copy(stored_in.at[k], stored.at[k], in_sem.at[k]) for k in range(count)]
    for load in loads:
        load.start()
    saves = []
    for k, load in enumerate(loads):
        load.wait()
        value = section_decay * store[k] + time_step * stored[k]
        store_next[k] = value
        fields_next[k] = fields[k] + section_gain * value
        saves.append(pltpu.make_async_copy(store_next.at[k], store_out.at[k], s_sem.at[k]))
        saves.append(pltpu.make_async_copy(fields_next.at[k], fields_out.at[k], f_sem.at[k]))
        saves[-2].start()
        saves[-1].start()
    for save in saves:
        save.wait()


def on_device(fields, store, mean, sound, slot, turns, offs, n_blk, n_span):
    per_theta, per_span = turns.shape
    assert per_theta == 1 and n_blk % 2 == 0
    elems = slot.shape[0]
    axial = elems // per_span
    w_hi, w_lo = (jnp.asarray(t) for t in derivative_tables())
    pick, turn, put = (jnp.asarray(t) for t in turn_tables())
    vmem = pl.BlockSpec(memory_space=pltpu.VMEM)
    hbm = pl.BlockSpec(memory_space=pl.ANY)
    smem = pl.BlockSpec(memory_space=pltpu.SMEM)
    dma = pltpu.SemaphoreType.DMA
    stored = pl.pallas_call(
        functools.partial(kernel, n_blk, n_span, per_span, axial),
        out_shape=jax.ShapeDtypeStruct((48, NODES, elems), F32),
        in_specs=[hbm] * 3 + [vmem] + [smem] * 2 + [hbm] * 5,
        out_specs=hbm,
        scratch_shapes=[
            pltpu.VMEM(fields.shape, F32),
            pltpu.VMEM((9, OFF + ROWS + 32, elems), F32),
            pltpu.VMEM((elems, elems), BF16),
            pltpu.VMEM((6 * ROWS, 5 * elems), BF16),
            pltpu.VMEM((5, ROWS, elems), F32),
            pltpu.VMEM((2, 7 * FACE + 1, elems), F32),
            pltpu.VMEM((2, 7 * FACE + 1, elems), F32),
            pltpu.VMEM((7 * FACE + 1, elems), F32),
            pltpu.VMEM((2, REST, elems), F32),
            pltpu.VMEM((2, REST, elems), F32),
            pltpu.VMEM((2, 5 * REST, elems), F32),
            pltpu.VMEM((2, 5 * REST, elems), F32),
            pltpu.VMEM((2, 5 * REST, elems), F32),
            pltpu.VMEM((5, FROWS // 2, elems), F32),
            pltpu.VMEM((2, 1, elems), jnp.int32),
            pltpu.VMEM((2, elems, elems), BF16),
            pltpu.VMEM((2, 7, FROWS, axial), F32),
            pltpu.VMEM((2, 7, FROWS, axial), F32),
            pltpu.VMEM((7, ROWS, axial), F32),
            pltpu.VMEM((FROWS // 2, 128), F32),
            pltpu.VMEM((n_blk - 1, FROWS // 2, 128), F32),
            pltpu.VMEM((FROWS, 128), F32),
            pltpu.VMEM((2 * FROWS, 5 * 128), F32),
            pltpu.VMEM(fields.shape, F32),
            pltpu.VMEM(mean.shape, F32),
            pltpu.VMEM(sound.shape, F32),
            *(pltpu.VMEM(t.shape, BF16) for t in (w_hi, w_lo, pick, turn, put)),
            dma((2, len(GROUPS))), dma((2, len(GROUPS))), dma((2,)), dma((2,)), dma((2, 2)), dma((2, 2)),
            dma((2,)), dma((2,)), dma((2,)), dma((2,)),
            dma((n_blk - 1,)), dma((n_blk - 1,)), dma((9,)), dma((3,)),
            pltpu.SemaphoreType.REGULAR, pltpu.SemaphoreType.REGULAR,
        ],
        compiler_params=pltpu.CompilerParams(collective_id=0, has_side_effects=True),
    )(fields, mean, sound, slot.reshape(1, elems), turns, offs, w_hi, w_lo, pick, turn, put)
    shape = jax.ShapeDtypeStruct(fields.shape, F32)
    count = fields.shape[0]
    return pl.pallas_call(
        finish,
        out_shape=(shape, shape),
        in_specs=[hbm, vmem, vmem],
        out_specs=(hbm, hbm),
        scratch_shapes=[pltpu.VMEM(fields.shape, F32)] * 3 + [dma((count,))] * 3,
        compiler_params=pltpu.CompilerParams(vmem_limit_bytes=50 * 2**20),
    )(stored, fields, store)


def solution(mesh):
    whole = P(None, None, ("blk", "span"))
    in_specs = (
        whole, whole, whole, P(None, ("blk", "span")), P(("blk", "span")), P("blk", "span"), P("span"),
    )
    body = functools.partial(on_device, n_blk=mesh.shape["blk"], n_span=mesh.shape["span"])
    return jax.shard_map(
        body, mesh=mesh, in_specs=in_specs, out_specs=(whole, whole), check_vma=False
    )
```

```python
import functools

import jax
import jax.numpy as jnp
import numpy as np
from jax import lax
from jax.experimental import pallas as pl
from jax.experimental.pallas import tpu as pltpu
from jax.sharding import PartitionSpec as P

ORDER = 4
N1 = ORDER + 1
FACE = N1 * N1
NODES = N1**3
ROWS = 128
OFF = 32
FROWS = 32
GROUPS = ((0, 9), (9, 17), (17, 25))
FIRST = GROUPS[0][1]
REST = FACE - FIRST
SENT = ((0, 1, 2, 3, 4, 5, 8), (0, 1, 2, 3, 4, 6, 8), (0, 1, 2, 3, 4, 7, 8))

section_decay = -567301805773.0 / 1357537059087.0
section_gain = 5161836677717.0 / 13612068292357.0
time_step = 0.05
metric_scale = (1.0, 1.5, 0.75)
end_weight = 0.1
MESH = pl.DeviceIdType.MESH
F32 = jnp.float32
BF16 = jnp.bfloat16


def lobatto_slopes():
    r = np.sqrt(3.0 / 7.0)
    x = np.array([-1.0, -r, 0.0, r, 1.0])
    n = x.shape[0]
    d = np.zeros((n, n))
    for i in range(n):
        for j in range(n):
            if i == j:
                d[i, j] = sum(1.0 / (x[i] - x[m]) for m in range(n) if m != i)
            else:
                a = np.prod([x[i] - x[m] for m in range(n) if m != i])
                b = np.prod([x[j] - x[m] for m in range(n) if m != j])
                d[i, j] = a / (b * (x[i] - x[j]))
    return d


def derivative_tables():
    slopes = lobatto_slopes().astype(np.float32).astype(np.float64)
    eye = np.eye(N1)
    full = np.zeros((ROWS, 3 * ROWS))
    for d in range(3):
        mats = [eye, eye, eye]
        mats[d] = slopes
        big = np.kron(np.kron(mats[0], mats[1]), mats[2])
        full[:NODES, d * ROWS : d * ROWS + NODES] = -metric_scale[d] * big
    hi = np.asarray(full, np.float32).astype(jnp.bfloat16)
    lo = (full - hi.astype(np.float64)).astype(np.float32).astype(jnp.bfloat16)
    return np.concatenate([hi, hi], axis=1), lo


def turn_tables():
    base = np.arange(FACE).reshape(N1, N1)
    pick = np.zeros((9 * FROWS, ROWS), np.float32)
    turn = np.zeros((8 * FROWS, FROWS), np.float32)
    put = np.zeros((ROWS, 2 * FROWS), np.float32)
    for n in range(FACE):
        pick[n, N1 * n + N1 - 1] = 1
        put[N1 * n + N1 - 1, n] = 1
        put[N1 * n, FROWS + n] = 1
    for o in range(8):
        fwd = base.T if o & 4 else base
        fwd = fwd[::-1] if o & 1 else fwd
        fwd = fwd[:, ::-1] if o & 2 else fwd
        inv = base[:, ::-1] if o & 2 else base
        inv = inv[::-1] if o & 1 else inv
        inv = inv.T if o & 4 else inv
        for n in range(FACE):
            pick[(o + 1) * FROWS + n, N1 * inv.reshape(-1)[n]] = 1
            turn[o * FROWS + n, fwd.reshape(-1)[n]] = 1
    return tuple(t.astype(jnp.bfloat16) for t in (pick, turn, put))


def split(x):
    hi = x.astype(BF16)
    return hi, (x - hi.astype(F32)).astype(BF16)


def dot(a, b):
    return jnp.dot(a, b, preferred_element_type=F32)


def dot_t(a, b):
    return lax.dot_general(a, b, (((1,), (1,)), ((), ())), preferred_element_type=F32)


def flux(state, d):
    q, m, c = state[:5], state[5], state[6]
    cu, cp = c * q[1 + d], c * q[4]
    out = [m * v for v in q]
    out[0] = out[0] + cu
    out[1 + d] = out[1 + d] + cp
    out[4] = out[4] + cu
    return out


def correction(own, outer, sign, d):
    w = 0.5 * metric_scale[d] / end_weight
    reach = jnp.maximum(jnp.abs(own[5]) + own[6], jnp.abs(outer[5]) + outer[6])
    fo, fx = flux(own, d), flux(outer, d)
    return [w * (sign * (fo[k] - fx[k]) + reach * (outer[k] - own[k])) for k in range(5)]


def merge(q, m, c, reach, d):
    return [f + reach * v for f, v in zip(flux([*q, m, c], d), q)]


def kernel(
    n_blk, n_span, per_span, axial, fields_in, mean_in, sound_in, slot, turns, offs, w_hi_in, w_lo_in,
    pick_in, turn_in, put_in,
    out_hbm, out, e, perm, fb, rates, th_send, th_recv, th_out, rate_send, rate_recv, up_send, up_recv, up_own, fix, far_slot, cross, sp_send, sp_recv, sp_rows, pk,
    gath, own_face, slide, fields, mean, sound, w_hi, w_lo, pick, turn, put,
    th_ss, th_rs, ra_ss, ra_rs, up_ss, up_rs, sl_ss, sl_rs, sp_ss, sp_rs, if_ss, if_rs, loaded, saved, ready, near,
):
    elems = per_span * axial
    half = axial // 2
    blk, slab = lax.axis_index("blk"), lax.axis_index("span")
    up, down = lax.rem(blk + 1, n_blk), lax.rem(blk + n_blk - 1, n_blk)
    right, left = lax.rem(slab + 1, n_span), lax.rem(slab + n_span - 1, n_span)

    first = pl.ds(0, 1)
    pairs = (
        (mean_in.at[first], mean.at[first]), (sound_in, sound), (fields_in, fields),
        (mean_in.at[pl.ds(1, 2)], mean.at[pl.ds(1, 2)]), (w_hi_in, w_hi), (w_lo_in, w_lo),
        (pick_in, pick), (turn_in, turn), (put_in, put),
    )
    loads = [pltpu.make_async_copy(a, b, loaded.at[n]) for n, (a, b) in enumerate(pairs)]
    for load in loads:
        load.start()
    even = lax.rem(blk, 2) == 0
    odd = jnp.logical_not(even)
    barrier = pltpu.get_barrier_semaphore()

    def greet(sem, target, cond):
        @pl.when(cond)
        def _():
            pl.semaphore_signal(sem, inc=1, device_id={"blk": target}, device_id_type=MESH)

    for k in range(1, n_blk):
        greet(barrier, lax.rem(blk + k, n_blk), blk + k < n_blk)
    greet(barrier, down, odd)
    for side in (right, left):
        pl.semaphore_signal(barrier, inc=1, device_id={"span": side}, device_id_type=MESH)

    last = NODES - FACE
    theta_own = [fields.at[k] for k in range(5)] + [mean.at[0], sound]
    near_side = lax.rem(blk, 2)
    far_side = 1 - near_side
    near_blk = jnp.where(even, up, down)
    far_blk = jnp.where(even, down, up)
    tail = blk == n_blk - 1
    wrap = jnp.logical_or(blk == 0, tail)
    inner = jnp.logical_not(wrap)

    def remote(src, dst, ss, rs, target):
        return pltpu.make_async_remote_copy(
            src_ref=src, dst_ref=dst, send_sem=ss, recv_sem=rs, device_id=target,
            device_id_type=MESH,
        )

    def flow(side, target):
        to = {"blk": target}
        slot_copy = remote(slot, far_slot.at[side], sl_ss.at[side], sl_rs.at[side], to)
        rate = remote(rate_send.at[side], rate_recv.at[side], ra_ss.at[side], ra_rs.at[side], to)
        full = []
        for g, (a, b) in enumerate(GROUPS):
            r = slice(7 * a + (g > 0), 7 * b + 1)
            full.append(remote(th_send.at[side, r], th_recv.at[side, r], th_ss.at[side, g], th_rs.at[side, g], to))
        half_size = 5 * REST // 2
        part = []
        for g in range(2):
            r = slice(g * half_size, (g + 1) * half_size)
            part.append(remote(up_send.at[side, r], up_recv.at[side, r], up_ss.at[side, g], up_rs.at[side, g], to))
        return slot_copy, rate, full, part

    def send(cond, copies, held=None):
        @pl.when(cond)
        def _():
            if held is not None:
                pl.semaphore_wait(held, 1)
            for copy in copies:
                copy.start()

    pl.semaphore_wait(barrier, blk + jnp.where(even, 1, 0) + 2)
    greet(near, down, jnp.logical_and(even, blk > 0))
    for k in range(1, n_blk):
        greet(ready, lax.rem(blk + n_blk - k, n_blk), jnp.logical_and(blk >= k, even) if k == 1 else blk >= k)
    near_slot, near_rate, near_full, near_part = flow(near_side, near_blk)
    far_slot_copy, far_rate, far_full, far_part = flow(far_side, far_blk)
    for load in loads[:2]:
        load.wait()
    for side, at in enumerate((last, 0)):
        rows = slice(at + FIRST, at + FACE)
        rate_send[side] = jnp.abs(mean[0, rows]) + sound[rows]
    near_slot.start()
    near_rate.start()
    low_far = jnp.logical_or(jnp.logical_and(even, inner), tail)
    send(low_far, [far_slot_copy, far_rate])
    loads[2].wait()
    for g, (a, b) in enumerate(GROUPS):
        for n, ref in enumerate(theta_own):
            at = 7 * a + (g > 0) + n * (b - a)
            th_send[0, at : at + b - a] = ref[last + a : last + b]
            th_send[1, at : at + b - a] = ref[a:b]
    send(tail, [far_full[0]])
    near_full[0].start()
    send(jnp.logical_and(even, inner), [far_full[0]])

    rows_i = lax.broadcasted_iota(jnp.int32, (elems, elems), 0)
    perm[...] = jnp.where(rows_i == slot[...], 1.0, 0.0).astype(BF16)


    def link(side):
        hi, lo = split(jnp.broadcast_to(far_slot[side].astype(F32), (8, elems)))
        source = (dot_t(hi, perm[...]) + dot_t(lo, perm[...]))[:1].astype(jnp.int32)
        cross[side] = jnp.where(rows_i == source, 1.0, 0.0).astype(BF16)

    def blend(side):
        sgn = jnp.where(side == 0, 1.0, -1.0)
        hi, lo = split(rate_recv[1 - side])
        there = dot(hi, cross[1 - side]) + dot(lo, cross[1 - side])
        reach = sgn * jnp.maximum(rate_send[side], there)
        for g, (a, b) in enumerate(GROUPS[1:]):
            at = 7 * a + 1
            own = [th_send[side, at + n * (b - a) : at + (n + 1) * (b - a)] for n in range(7)]
            speed = reach[a - FIRST : b - FIRST]
            for sign, ref in ((1.0, up_send), (-1.0, up_own)):
                for k, v in enumerate(merge(own[:5], own[5], own[6], sign * speed, 0)):
                    to = 5 * (a - FIRST) + k * (b - a)
                    ref[side, to : to + b - a] = v

    in_near = flow(far_side, near_blk)
    in_far = flow(near_side, far_blk)
    def settle_near():
        in_near[0].wait_recv()
        link(far_side)
        in_near[1].wait_recv()
        blend(near_side)
        near_part[0].start()
        near_part[1].start()


    for load in loads[3:]:
        load.wait()
    cells = 2 * per_span
    lane = lax.broadcasted_iota(jnp.int32, (1, 128), 1)
    lane_f, lane_cell = lane // cells, lax.rem(lane, cells)
    lane_s = lax.rem(lane_cell, per_span)
    stator = lane_cell < per_span
    code = jnp.zeros((1, 128), jnp.int32)
    turn_by = jnp.zeros((1, 128), jnp.int32)
    for s in range(per_span):
        code = jnp.where(lane_s == s, turns[0, s], code)
        turn_by = jnp.where(lane_s == s, offs[s], turn_by)
    place = jnp.zeros((1, 128), jnp.int32)
    for c in range(cells):
        at = (c % per_span) * axial + half - 1 + c // per_span
        place = jnp.where(lane_cell == c, slot[:, at : at + 1], place)
    elem = lax.broadcasted_iota(jnp.int32, (elems, 128), 0)
    own_side = jnp.where(elem == place, 1.0, 0.0).astype(BF16)
    state = [fields.at[k] for k in range(5)] + [mean.at[d] for d in range(3)] + [sound]
    z = jnp.zeros((NODES, 128), F32)
    for n, f in enumerate(SENT[2]):
        hi, lo = split(state[f][...])
        z = jnp.where(lane_f == n, dot(hi, own_side) + dot(lo, own_side), z)
    hi, lo = split(jnp.concatenate([z, jnp.zeros((ROWS - NODES, 128), F32)], axis=0))
    picked = dot(pick[...], hi) + dot(pick[...], lo)
    own_face[...] = jnp.where(stator, picked[:FROWS], picked[FROWS : 2 * FROWS])
    packet = picked[:FROWS]
    for o in range(8):
        part = picked[(o + 1) * FROWS : (o + 2) * FROWS]
        packet = jnp.where(jnp.logical_and(jnp.logical_not(stator), code == o), part, packet)
    half_rows = FROWS // 2
    pk[...] = jnp.where(lane < 64, packet[:half_rows], pltpu.roll(packet[half_rows:], 64, 1))
    if_copies = [
        remote(pk, gath.at[k - 1], if_ss.at[k - 1], if_rs.at[k - 1], {"blk": lax.rem(blk + k, n_blk)})
        for k in range(1, n_blk)
    ]
    for k, copy in enumerate(if_copies, 1):
        send(blk + k >= n_blk, [copy])
    send(jnp.logical_and(odd, inner), [far_slot_copy, far_rate, far_full[0]], near)

    def gather(f, value):
        hi, lo = split(value)
        e[f, :OFF] = jnp.zeros((OFF, elems), F32)
        e[f, OFF + 120 :] = jnp.zeros((e.shape[1] - OFF - 120, elems), F32)
        e[f, OFF : OFF + NODES] = dot(hi, perm[...]) + dot(lo, perm[...])

    for f in range(9):
        gather(f, state[f][...])

    block = slice(OFF, OFF + ROWS)
    for n, f in enumerate(SENT[1]):
        for i in range(N1):
            at = OFF + i * FACE
            sp_send[0, n, i * N1 : (i + 1) * N1] = e[f, at + 20 : at + 25, elems - axial :]
            sp_send[1, n, i * N1 : (i + 1) * N1] = e[f, at : at + 5, :axial]
    sp_up = remote(sp_send.at[0], sp_recv.at[0], sp_ss.at[0], sp_rs.at[0], {"span": right})
    sp_dn = remote(sp_send.at[1], sp_recv.at[1], sp_ss.at[1], sp_rs.at[1], {"span": left})
    inner_hi, inner_lo = slab < n_span - 1, slab > 0
    send(inner_hi, [sp_up])
    send(inner_lo, [sp_dn])

    above = n_blk - 1 - blk - jnp.where(even, 1, 0)

    @pl.when(above > 0)
    def _():
        pl.semaphore_wait(ready, above)

    send(blk == 0, [far_slot_copy, far_rate, far_full[0]])
    for k, copy in enumerate(if_copies, 1):
        send(blk + k < n_blk, [copy])
    settle_near()
    def settle_far():
        in_far[0].wait_recv()
        link(near_side)
        in_far[1].wait_recv()
        blend(far_side)
        far_part[0].start()
        far_part[1].start()

    pl.when(inner)(settle_far)

    for s in range(per_span):
        ln = slice(s * axial, (s + 1) * axial)
        for d in range(3):
            for k, v in enumerate(flux([e[f, block, ln] for f in SENT[d]], d)):
                hi, lo = split(v)
                at = slice(k * elems + s * axial, k * elems + (s + 1) * axial)
                fb[d * ROWS : (d + 1) * ROWS, at] = hi
                fb[(3 + d) * ROWS : (4 + d) * ROWS, at] = lo
    for k in range(5):
        at = slice(k * elems, (k + 1) * elems)
        rates[k] = dot(w_hi[...], fb[:, at]) + dot(w_lo[...], fb[: 3 * ROWS, at])


    pl.when(wrap)(settle_far)
    row = lax.broadcasted_iota(jnp.int32, (ROWS, axial), 0)
    a_id = lax.broadcasted_iota(jnp.int32, (ROWS, axial), 1)
    k_id = lax.rem(row // N1, N1)

    @pl.when(inner_hi)
    def _():
        sp_up.wait_send()
        sp_dn.wait_recv()

    @pl.when(inner_lo)
    def _():
        sp_dn.wait_send()
        sp_up.wait_recv()

    for n in range(7):
        for i in range(N1):
            at = i * FACE
            sp_rows[n, at : at + 5] = sp_recv[0, n, i * N1 : (i + 1) * N1]
            sp_rows[n, at + 20 : at + 25] = sp_recv[1, n, i * N1 : (i + 1) * N1]
    low = k_id == 0
    face = jnp.logical_and(jnp.logical_or(low, k_id == N1 - 1), row < NODES)
    sign = jnp.where(low, -1.0, 1.0)
    for s in range(per_span):
        ln = slice(s * axial, (s + 1) * axial)
        own = [e[f, block, ln] for f in SENT[1]]
        outer = []
        for n, f in enumerate(SENT[1]):
            wall = -own[n] if n == 2 else own[n]
            if s == 0:
                lo_v = jnp.where(slab > 0, sp_rows[n], wall)
            else:
                lo_v = e[f, OFF + 20 : OFF + 20 + ROWS, (s - 1) * axial : s * axial]
            if s == per_span - 1:
                hi_v = jnp.where(slab < n_span - 1, sp_rows[n], wall)
            else:
                hi_v = e[f, OFF - 20 : OFF - 20 + ROWS, (s + 1) * axial : (s + 2) * axial]
            outer.append(jnp.where(low, lo_v, hi_v))
        for k, v in enumerate(correction(own, outer, sign, 1)):
            rates[k, :, ln] += jnp.where(face, v, 0.0)

    l_id = lax.rem(row, N1)
    low = l_id == 0
    face = jnp.logical_and(jnp.logical_or(low, l_id == N1 - 1), row < NODES)
    sign = jnp.where(low, -1.0, 1.0)
    slides = a_id == jnp.where(low, half, half - 1)
    ends = a_id == jnp.where(low, 0, axial - 1)
    for s in range(per_span):
        ln = slice(s * axial, (s + 1) * axial)
        own = [e[f, block, ln] for f in SENT[2]]
        outer = []
        for n, f in enumerate(SENT[2]):
            lo_v = pltpu.roll(e[f, OFF + 4 : OFF + 4 + ROWS, ln], 1, 1)
            hi_v = pltpu.roll(e[f, OFF - 4 : OFF - 4 + ROWS, ln], axial - 1, 1)
            v = jnp.where(slides, own[n], jnp.where(low, lo_v, hi_v))
            outer.append(jnp.where(ends, own[n] if n > 4 else 0.0, v))
        for k, v in enumerate(correction(own, outer, sign, 2)):
            rates[k, :, ln] += jnp.where(face, v, 0.0)

    for k in range(5):
        hi, lo = split(rates[k])
        out[k] = (dot_t(hi, perm[...]) + dot_t(lo, perm[...]))[:NODES]

    for copy in if_copies:
        copy.wait()
    steps = jnp.where(stator, turn_by, lax.rem(n_blk - turn_by, n_blk))
    chosen = pk[...]
    for k in range(1, n_blk):
        chosen = jnp.where(steps == k, gath[k - 1], chosen)
    chosen = jnp.concatenate([chosen, pltpu.roll(chosen, 64, 1)], axis=0)
    hi, lo = split(chosen)
    parts = dot(turn[...], hi) + dot(turn[...], lo)
    for o in range(8):
        chosen = jnp.where(jnp.logical_and(stator, code == o), parts[o * FROWS : (o + 1) * FROWS], chosen)
    outer = jnp.where(stator, pltpu.roll(chosen, 128 - per_span, 1), pltpu.roll(chosen, per_span, 1))

    def traces(x):
        return [x if n == 0 else pltpu.roll(x, 128 - n * cells, 1) for n in range(7)]

    sgn = jnp.where(stator, 1.0, -1.0)
    for k, v in enumerate(correction(traces(own_face[...]), traces(outer), sgn, 2)):
        at = slice(k * 128, (k + 1) * 128)
        slide[:FROWS, at] = jnp.where(lane < per_span, v, 0.0)
        slide[FROWS:, at] = jnp.where(jnp.logical_and(lane >= per_span, lane < cells), v, 0.0)
    hi, lo = split(slide[...])
    jumps = dot(put[...], hi) + dot(put[...], lo)
    for k in range(5):
        hi, lo = split(jumps[:, k * 128 : (k + 1) * 128])
        out[k] += (dot_t(hi, own_side) + dot_t(lo, own_side))[:NODES]

    mid = pltpu.make_async_copy(out.at[:, 32:96], out_hbm.at[:5, 32:96], saved.at[0])
    mid.start()

    def add(side, a, b):
        for at, cond in ((0, side == 0), (last, side == 1)):
            @pl.when(cond)
            def _():
                for k in range(5):
                    out[k, at + a : at + b] += fix[k, : b - a]

    def theta(side, g, copy):
        copy.wait_recv()
        a, b = GROUPS[g]
        at = 7 * a + (g > 0)
        hi, lo = split(th_recv[side, at : at + 7 * (b - a)])
        th_out[: 7 * (b - a)] = dot(hi, cross[side]) + dot(lo, cross[side])
        own = [th_send[1 - side, at + n * (b - a) : at + (n + 1) * (b - a)] for n in range(7)]
        outer = [th_out[n * (b - a) : (n + 1) * (b - a)] for n in range(7)]
        sgn = jnp.where(side == 0, -1.0, 1.0)
        for k, v in enumerate(correction(own, outer, sgn, 0)):
            fix[k, : b - a] = v
        add(side, a, b)

    def blended(side, g, copy):
        copy.wait_recv()
        a, b = GROUPS[g]
        at = 5 * (a - FIRST)
        hi, lo = split(up_recv[side, at : at + 5 * (b - a)])
        there = dot(hi, cross[side]) + dot(lo, cross[side])
        w = 0.5 * metric_scale[0] / end_weight * jnp.where(side == 0, -1.0, 1.0)
        for k in range(5):
            n = slice(k * (b - a), (k + 1) * (b - a))
            fix[k, : b - a] = w * (up_own[1 - side, at + k * (b - a) : at + (k + 1) * (b - a)] - there[n])
        add(side, a, b)

    theta(far_side, 0, in_near[2][0])
    theta(near_side, 0, in_far[2][0])

    blended(far_side, 1, in_near[3][0])
    for g in (1, 2):
        blended(near_side, g, in_far[3][g - 1])
    blended(far_side, 2, in_near[3][1])

    lows = pltpu.make_async_copy(out.at[:, :32], out_hbm.at[:5, :32], saved.at[1])
    highs = pltpu.make_async_copy(out.at[:, 96:], out_hbm.at[:5, 96:], saved.at[2])
    lows.start()
    highs.start()
    for copy in (near_slot, near_rate, near_full[0], *near_part, far_slot_copy, far_rate, far_full[0], *far_part):
        copy.wait_send()
    for copy in (mid, lows, highs):
        copy.wait()


def finish(stored_in, fields, store, fields_out, store_out, stored, fields_next, store_next, in_sem, f_sem, s_sem):
    count = stored.shape[0]
    loads = [pltpu.make_async_copy(stored_in.at[k], stored.at[k], in_sem.at[k]) for k in range(count)]
    for load in loads:
        load.start()
    saves = []
    for k, load in enumerate(loads):
        load.wait()
        value = section_decay * store[k] + time_step * stored[k]
        store_next[k] = value
        fields_next[k] = fields[k] + section_gain * value
        saves.append(pltpu.make_async_copy(store_next.at[k], store_out.at[k], s_sem.at[k]))
        saves.append(pltpu.make_async_copy(fields_next.at[k], fields_out.at[k], f_sem.at[k]))
        saves[-2].start()
        saves[-1].start()
    for save in saves:
        save.wait()


def on_device(fields, store, mean, sound, slot, turns, offs, n_blk, n_span):
    per_theta, per_span = turns.shape
    assert per_theta == 1 and n_blk % 2 == 0
    elems = slot.shape[0]
    axial = elems // per_span
    w_hi, w_lo = (jnp.asarray(t) for t in derivative_tables())
    pick, turn, put = (jnp.asarray(t) for t in turn_tables())
    vmem = pl.BlockSpec(memory_space=pltpu.VMEM)
    hbm = pl.BlockSpec(memory_space=pl.ANY)
    smem = pl.BlockSpec(memory_space=pltpu.SMEM)
    dma = pltpu.SemaphoreType.DMA
    stored = pl.pallas_call(
        functools.partial(kernel, n_blk, n_span, per_span, axial),
        out_shape=jax.ShapeDtypeStruct((48, NODES, elems), F32),
        in_specs=[hbm] * 3 + [vmem] + [smem] * 2 + [hbm] * 5,
        out_specs=hbm,
        scratch_shapes=[
            pltpu.VMEM(fields.shape, F32),
            pltpu.VMEM((9, OFF + ROWS + 32, elems), F32),
            pltpu.VMEM((elems, elems), BF16),
            pltpu.VMEM((6 * ROWS, 5 * elems), BF16),
            pltpu.VMEM((5, ROWS, elems), F32),
            pltpu.VMEM((2, 7 * FACE + 1, elems), F32),
            pltpu.VMEM((2, 7 * FACE + 1, elems), F32),
            pltpu.VMEM((7 * FACE + 1, elems), F32),
            pltpu.VMEM((2, REST, elems), F32),
            pltpu.VMEM((2, REST, elems), F32),
            pltpu.VMEM((2, 5 * REST, elems), F32),
            pltpu.VMEM((2, 5 * REST, elems), F32),
            pltpu.VMEM((2, 5 * REST, elems), F32),
            pltpu.VMEM((5, FROWS // 2, elems), F32),
            pltpu.VMEM((2, 1, elems), jnp.int32),
            pltpu.VMEM((2, elems, elems), BF16),
            pltpu.VMEM((2, 7, FROWS, axial), F32),
            pltpu.VMEM((2, 7, FROWS, axial), F32),
            pltpu.VMEM((7, ROWS, axial), F32),
            pltpu.VMEM((FROWS // 2, 128), F32),
            pltpu.VMEM((n_blk - 1, FROWS // 2, 128), F32),
            pltpu.VMEM((FROWS, 128), F32),
            pltpu.VMEM((2 * FROWS, 5 * 128), F32),
            pltpu.VMEM(fields.shape, F32),
            pltpu.VMEM(mean.shape, F32),
            pltpu.VMEM(sound.shape, F32),
            *(pltpu.VMEM(t.shape, BF16) for t in (w_hi, w_lo, pick, turn, put)),
            dma((2, len(GROUPS))), dma((2, len(GROUPS))), dma((2,)), dma((2,)), dma((2, 2)), dma((2, 2)),
            dma((2,)), dma((2,)), dma((2,)), dma((2,)),
            dma((n_blk - 1,)), dma((n_blk - 1,)), dma((9,)), dma((3,)),
            pltpu.SemaphoreType.REGULAR, pltpu.SemaphoreType.REGULAR,
        ],
        compiler_params=pltpu.CompilerParams(collective_id=0, has_side_effects=True),
    )(fields, mean, sound, slot.reshape(1, elems), turns, offs, w_hi, w_lo, pick, turn, put)
    shape = jax.ShapeDtypeStruct(fields.shape, F32)
    count = fields.shape[0]
    return pl.pallas_call(
        finish,
        out_shape=(shape, shape),
        in_specs=[hbm, vmem, vmem],
        out_specs=(hbm, hbm),
        scratch_shapes=[pltpu.VMEM(fields.shape, F32)] * 3 + [dma((count,))] * 3,
        compiler_params=pltpu.CompilerParams(vmem_limit_bytes=50 * 2**20),
    )(stored, fields, store)


def solution(mesh):
    whole = P(None, None, ("blk", "span"))
    in_specs = (
        whole, whole, whole, P(None, ("blk", "span")), P(("blk", "span")), P("blk", "span"), P("span"),
    )
    body = functools.partial(on_device, n_blk=mesh.shape["blk"], n_span=mesh.shape["span"])
    return jax.shard_map(
        body, mesh=mesh, in_specs=in_specs, out_specs=(whole, whole), check_vma=False
    )
```

```python
import functools

import jax
import jax.numpy as jnp
import numpy as np
from jax import lax
from jax.experimental import pallas as pl
from jax.experimental.pallas import tpu as pltpu
from jax.sharding import PartitionSpec as P

ORDER = 4
N1 = ORDER + 1
FACE = N1 * N1
NODES = N1**3
ROWS = 128
OFF = 32
FROWS = 32
GROUPS = ((0, 9), (9, 17), (17, 25))
FIRST = GROUPS[0][1]
REST = FACE - FIRST
SENT = ((0, 1, 2, 3, 4, 5, 8), (0, 1, 2, 3, 4, 6, 8), (0, 1, 2, 3, 4, 7, 8))

section_decay = -567301805773.0 / 1357537059087.0
section_gain = 5161836677717.0 / 13612068292357.0
time_step = 0.05
metric_scale = (1.0, 1.5, 0.75)
end_weight = 0.1
MESH = pl.DeviceIdType.MESH
F32 = jnp.float32
BF16 = jnp.bfloat16


def lobatto_slopes():
    r = np.sqrt(3.0 / 7.0)
    x = np.array([-1.0, -r, 0.0, r, 1.0])
    n = x.shape[0]
    d = np.zeros((n, n))
    for i in range(n):
        for j in range(n):
            if i == j:
                d[i, j] = sum(1.0 / (x[i] - x[m]) for m in range(n) if m != i)
            else:
                a = np.prod([x[i] - x[m] for m in range(n) if m != i])
                b = np.prod([x[j] - x[m] for m in range(n) if m != j])
                d[i, j] = a / (b * (x[i] - x[j]))
    return d


def derivative_tables():
    slopes = lobatto_slopes().astype(np.float32).astype(np.float64)
    eye = np.eye(N1)
    full = np.zeros((ROWS, 3 * ROWS))
    for d in range(3):
        mats = [eye, eye, eye]
        mats[d] = slopes
        big = np.kron(np.kron(mats[0], mats[1]), mats[2])
        full[:NODES, d * ROWS : d * ROWS + NODES] = -metric_scale[d] * big
    hi = np.asarray(full, np.float32).astype(jnp.bfloat16)
    lo = (full - hi.astype(np.float64)).astype(np.float32).astype(jnp.bfloat16)
    return np.concatenate([hi, hi], axis=1), lo


def turn_tables():
    base = np.arange(FACE).reshape(N1, N1)
    pick = np.zeros((9 * FROWS, ROWS), np.float32)
    turn = np.zeros((8 * FROWS, FROWS), np.float32)
    put = np.zeros((ROWS, 2 * FROWS), np.float32)
    for n in range(FACE):
        pick[n, N1 * n + N1 - 1] = 1
        put[N1 * n + N1 - 1, n] = 1
        put[N1 * n, FROWS + n] = 1
    for o in range(8):
        fwd = base.T if o & 4 else base
        fwd = fwd[::-1] if o & 1 else fwd
        fwd = fwd[:, ::-1] if o & 2 else fwd
        inv = base[:, ::-1] if o & 2 else base
        inv = inv[::-1] if o & 1 else inv
        inv = inv.T if o & 4 else inv
        for n in range(FACE):
            pick[(o + 1) * FROWS + n, N1 * inv.reshape(-1)[n]] = 1
            turn[o * FROWS + n, fwd.reshape(-1)[n]] = 1
    return tuple(t.astype(jnp.bfloat16) for t in (pick, turn, put))


def split(x):
    hi = x.astype(BF16)
    return hi, (x - hi.astype(F32)).astype(BF16)


def dot(a, b):
    return jnp.dot(a, b, preferred_element_type=F32)


def dot_t(a, b):
    return lax.dot_general(a, b, (((1,), (1,)), ((), ())), preferred_element_type=F32)


def shuffle(x, table):
    rows = x.shape[0]
    hi = x.astype(BF16).astype(F32)
    both = dot(jnp.concatenate([hi, x - hi], axis=0).astype(BF16), table)
    return both[:rows] + both[rows:]


def flux(state, d):
    q, m, c = state[:5], state[5], state[6]
    cu, cp = c * q[1 + d], c * q[4]
    out = [m * v for v in q]
    out[0] = out[0] + cu
    out[1 + d] = out[1 + d] + cp
    out[4] = out[4] + cu
    return out


def correction(own, outer, sign, d):
    w = 0.5 * metric_scale[d] / end_weight
    reach = jnp.maximum(jnp.abs(own[5]) + own[6], jnp.abs(outer[5]) + outer[6])
    fo, fx = flux(own, d), flux(outer, d)
    return [w * (sign * (fo[k] - fx[k]) + reach * (outer[k] - own[k])) for k in range(5)]


def merge(q, m, c, reach, d):
    return [f + reach * v for f, v in zip(flux([*q, m, c], d), q)]


def kernel(
    n_blk, n_span, per_span, axial, fields_in, mean_in, sound_in, slot, turns, offs, w_hi_in, w_lo_in,
    pick_in, turn_in, put_in,
    out_hbm, out, e, perm, fb, rates, th_send, th_recv, th_out, rate_send, rate_recv, up_send, up_recv, up_own, fix, far_slot, cross, sp_send, sp_recv, sp_rows, pk,
    gath, own_face, slide, fields, mean, sound, w_hi, w_lo, pick, turn, put,
    th_ss, th_rs, ra_ss, ra_rs, up_ss, up_rs, sl_ss, sl_rs, sp_ss, sp_rs, if_ss, if_rs, loaded, saved, ready, near,
):
    elems = per_span * axial
    half = axial // 2
    blk, slab = lax.axis_index("blk"), lax.axis_index("span")
    up, down = lax.rem(blk + 1, n_blk), lax.rem(blk + n_blk - 1, n_blk)
    right, left = lax.rem(slab + 1, n_span), lax.rem(slab + n_span - 1, n_span)

    first = pl.ds(0, 1)
    pairs = (
        (mean_in.at[first], mean.at[first]), (sound_in, sound), (fields_in, fields),
        (mean_in.at[pl.ds(1, 2)], mean.at[pl.ds(1, 2)]), (w_hi_in, w_hi), (w_lo_in, w_lo),
        (pick_in, pick), (turn_in, turn), (put_in, put),
    )
    loads = [pltpu.make_async_copy(a, b, loaded.at[n]) for n, (a, b) in enumerate(pairs)]
    for load in loads:
        load.start()
    even = lax.rem(blk, 2) == 0
    odd = jnp.logical_not(even)
    barrier = pltpu.get_barrier_semaphore()

    def greet(sem, target, cond):
        @pl.when(cond)
        def _():
            pl.semaphore_signal(sem, inc=1, device_id={"blk": target}, device_id_type=MESH)

    for k in range(1, n_blk):
        greet(barrier, lax.rem(blk + k, n_blk), blk + k < n_blk)
    greet(barrier, down, odd)
    for side in (right, left):
        pl.semaphore_signal(barrier, inc=1, device_id={"span": side}, device_id_type=MESH)

    last = NODES - FACE
    theta_own = [fields.at[k] for k in range(5)] + [mean.at[0], sound]
    near_side = lax.rem(blk, 2)
    far_side = 1 - near_side
    near_blk = jnp.where(even, up, down)
    far_blk = jnp.where(even, down, up)
    tail = blk == n_blk - 1
    wrap = jnp.logical_or(blk == 0, tail)
    inner = jnp.logical_not(wrap)

    def remote(src, dst, ss, rs, target):
        return pltpu.make_async_remote_copy(
            src_ref=src, dst_ref=dst, send_sem=ss, recv_sem=rs, device_id=target,
            device_id_type=MESH,
        )

    def flow(side, target):
        to = {"blk": target}
        slot_copy = remote(slot, far_slot.at[side], sl_ss.at[side], sl_rs.at[side], to)
        rate = remote(rate_send.at[side], rate_recv.at[side], ra_ss.at[side], ra_rs.at[side], to)
        full = []
        for g, (a, b) in enumerate(GROUPS):
            r = slice(7 * a + (g > 0), 7 * b + 1)
            full.append(remote(th_send.at[side, r], th_recv.at[side, r], th_ss.at[side, g], th_rs.at[side, g], to))
        half_size = 5 * REST // 2
        part = []
        for g in range(2):
            r = slice(g * half_size, (g + 1) * half_size)
            part.append(remote(up_send.at[side, r], up_recv.at[side, r], up_ss.at[side, g], up_rs.at[side, g], to))
        return slot_copy, rate, full, part

    def send(cond, copies, held=None):
        @pl.when(cond)
        def _():
            if held is not None:
                pl.semaphore_wait(held, 1)
            for copy in copies:
                copy.start()

    pl.semaphore_wait(barrier, blk + jnp.where(even, 1, 0) + 2)
    greet(near, down, jnp.logical_and(even, blk > 0))
    for k in range(1, n_blk):
        greet(ready, lax.rem(blk + n_blk - k, n_blk), jnp.logical_and(blk >= k, even) if k == 1 else blk >= k)
    near_slot, near_rate, near_full, near_part = flow(near_side, near_blk)
    far_slot_copy, far_rate, far_full, far_part = flow(far_side, far_blk)
    for load in loads[:2]:
        load.wait()
    for side, at in enumerate((last, 0)):
        rows = slice(at + FIRST, at + FACE)
        rate_send[side] = jnp.abs(mean[0, rows]) + sound[rows]
    near_slot.start()
    near_rate.start()
    low_far = jnp.logical_or(jnp.logical_and(even, inner), tail)
    send(low_far, [far_slot_copy, far_rate])
    loads[2].wait()
    for g, (a, b) in enumerate(GROUPS):
        for n, ref in enumerate(theta_own):
            at = 7 * a + (g > 0) + n * (b - a)
            th_send[0, at : at + b - a] = ref[last + a : last + b]
            th_send[1, at : at + b - a] = ref[a:b]
    send(tail, [far_full[0]])
    near_full[0].start()
    send(jnp.logical_and(even, inner), [far_full[0]])

    rows_i = lax.broadcasted_iota(jnp.int32, (elems, elems), 0)
    perm[...] = jnp.where(rows_i == slot[...], 1.0, 0.0).astype(BF16)


    def link(side):
        hi, lo = split(jnp.broadcast_to(far_slot[side].astype(F32), (8, elems)))
        source = (dot_t(hi, perm[...]) + dot_t(lo, perm[...]))[:1].astype(jnp.int32)
        cross[side] = jnp.where(rows_i == source, 1.0, 0.0).astype(BF16)

    def blend(side):
        sgn = jnp.where(side == 0, 1.0, -1.0)
        there = shuffle(rate_recv[1 - side], cross[1 - side])
        reach = sgn * jnp.maximum(rate_send[side], there)
        for g, (a, b) in enumerate(GROUPS[1:]):
            at = 7 * a + 1
            own = [th_send[side, at + n * (b - a) : at + (n + 1) * (b - a)] for n in range(7)]
            speed = reach[a - FIRST : b - FIRST]
            for sign, ref in ((1.0, up_send), (-1.0, up_own)):
                for k, v in enumerate(merge(own[:5], own[5], own[6], sign * speed, 0)):
                    to = 5 * (a - FIRST) + k * (b - a)
                    ref[side, to : to + b - a] = v

    in_near = flow(far_side, near_blk)
    in_far = flow(near_side, far_blk)
    def settle_near():
        in_near[0].wait_recv()
        link(far_side)
        in_near[1].wait_recv()
        blend(near_side)
        near_part[0].start()
        near_part[1].start()


    for load in loads[3:]:
        load.wait()
    cells = 2 * per_span
    lane = lax.broadcasted_iota(jnp.int32, (1, 128), 1)
    lane_f, lane_cell = lane // cells, lax.rem(lane, cells)
    lane_s = lax.rem(lane_cell, per_span)
    stator = lane_cell < per_span
    code = jnp.zeros((1, 128), jnp.int32)
    turn_by = jnp.zeros((1, 128), jnp.int32)
    for s in range(per_span):
        code = jnp.where(lane_s == s, turns[0, s], code)
        turn_by = jnp.where(lane_s == s, offs[s], turn_by)
    place = jnp.zeros((1, 128), jnp.int32)
    for c in range(cells):
        at = (c % per_span) * axial + half - 1 + c // per_span
        place = jnp.where(lane_cell == c, slot[:, at : at + 1], place)
    elem = lax.broadcasted_iota(jnp.int32, (elems, 128), 0)
    own_side = jnp.where(elem == place, 1.0, 0.0).astype(BF16)
    state = [fields.at[k] for k in range(5)] + [mean.at[d] for d in range(3)] + [sound]
    z = jnp.zeros((NODES, 128), F32)
    for n, f in enumerate(SENT[2]):
        hi, lo = split(state[f][...])
        z = jnp.where(lane_f == n, dot(hi, own_side) + dot(lo, own_side), z)
    hi, lo = split(jnp.concatenate([z, jnp.zeros((ROWS - NODES, 128), F32)], axis=0))
    picked = dot(pick[...], hi) + dot(pick[...], lo)
    own_face[...] = jnp.where(stator, picked[:FROWS], picked[FROWS : 2 * FROWS])
    packet = picked[:FROWS]
    for o in range(8):
        part = picked[(o + 1) * FROWS : (o + 2) * FROWS]
        packet = jnp.where(jnp.logical_and(jnp.logical_not(stator), code == o), part, packet)
    half_rows = FROWS // 2
    pk[...] = jnp.where(lane < 64, packet[:half_rows], pltpu.roll(packet[half_rows:], 64, 1))
    if_copies = [
        remote(pk, gath.at[k - 1], if_ss.at[k - 1], if_rs.at[k - 1], {"blk": lax.rem(blk + k, n_blk)})
        for k in range(1, n_blk)
    ]
    for k, copy in enumerate(if_copies, 1):
        send(blk + k >= n_blk, [copy])
    send(jnp.logical_and(odd, inner), [far_slot_copy, far_rate, far_full[0]], near)

    def gather(f, value):
        hi, lo = split(value)
        e[f, :OFF] = jnp.zeros((OFF, elems), F32)
        e[f, OFF + 120 :] = jnp.zeros((e.shape[1] - OFF - 120, elems), F32)
        e[f, OFF : OFF + NODES] = dot(hi, perm[...]) + dot(lo, perm[...])

    for f in range(9):
        gather(f, state[f][...])

    block = slice(OFF, OFF + ROWS)
    for n, f in enumerate(SENT[1]):
        for i in range(N1):
            at = OFF + i * FACE
            sp_send[0, n, i * N1 : (i + 1) * N1] = e[f, at + 20 : at + 25, elems - axial :]
            sp_send[1, n, i * N1 : (i + 1) * N1] = e[f, at : at + 5, :axial]
    sp_up = remote(sp_send.at[0], sp_recv.at[0], sp_ss.at[0], sp_rs.at[0], {"span": right})
    sp_dn = remote(sp_send.at[1], sp_recv.at[1], sp_ss.at[1], sp_rs.at[1], {"span": left})
    inner_hi, inner_lo = slab < n_span - 1, slab > 0
    send(inner_hi, [sp_up])
    send(inner_lo, [sp_dn])

    pl.when(odd)(settle_near)
    above = n_blk - 1 - blk - jnp.where(even, 1, 0)

    @pl.when(above > 0)
    def _():
        pl.semaphore_wait(ready, above)

    send(blk == 0, [far_slot_copy, far_rate, far_full[0]])
    for k, copy in enumerate(if_copies, 1):
        send(blk + k < n_blk, [copy])
    pl.when(even)(settle_near)
    def settle_far():
        in_far[0].wait_recv()
        link(near_side)
        in_far[1].wait_recv()
        blend(far_side)
        far_part[0].start()
        far_part[1].start()

    pl.when(inner)(settle_far)

    for s in range(per_span):
        ln = slice(s * axial, (s + 1) * axial)
        for d in range(3):
            for k, v in enumerate(flux([e[f, block, ln] for f in SENT[d]], d)):
                hi, lo = split(v)
                at = slice(k * elems + s * axial, k * elems + (s + 1) * axial)
                fb[d * ROWS : (d + 1) * ROWS, at] = hi
                fb[(3 + d) * ROWS : (4 + d) * ROWS, at] = lo
    for k in range(5):
        at = slice(k * elems, (k + 1) * elems)
        rates[k] = dot(w_hi[...], fb[:, at]) + dot(w_lo[...], fb[: 3 * ROWS, at])


    pl.when(wrap)(settle_far)
    row = lax.broadcasted_iota(jnp.int32, (ROWS, axial), 0)
    a_id = lax.broadcasted_iota(jnp.int32, (ROWS, axial), 1)
    k_id = lax.rem(row // N1, N1)

    @pl.when(inner_hi)
    def _():
        sp_up.wait_send()
        sp_dn.wait_recv()

    @pl.when(inner_lo)
    def _():
        sp_dn.wait_send()
        sp_up.wait_recv()

    for n in range(7):
        for i in range(N1):
            at = i * FACE
            sp_rows[n, at : at + 5] = sp_recv[0, n, i * N1 : (i + 1) * N1]
            sp_rows[n, at + 20 : at + 25] = sp_recv[1, n, i * N1 : (i + 1) * N1]
    low = k_id == 0
    face = jnp.logical_and(jnp.logical_or(low, k_id == N1 - 1), row < NODES)
    sign = jnp.where(low, -1.0, 1.0)
    for s in range(per_span):
        ln = slice(s * axial, (s + 1) * axial)
        own = [e[f, block, ln] for f in SENT[1]]
        outer = []
        for n, f in enumerate(SENT[1]):
            wall = -own[n] if n == 2 else own[n]
            if s == 0:
                lo_v = jnp.where(slab > 0, sp_rows[n], wall)
            else:
                lo_v = e[f, OFF + 20 : OFF + 20 + ROWS, (s - 1) * axial : s * axial]
            if s == per_span - 1:
                hi_v = jnp.where(slab < n_span - 1, sp_rows[n], wall)
            else:
                hi_v = e[f, OFF - 20 : OFF - 20 + ROWS, (s + 1) * axial : (s + 2) * axial]
            outer.append(jnp.where(low, lo_v, hi_v))
        for k, v in enumerate(correction(own, outer, sign, 1)):
            rates[k, :, ln] += jnp.where(face, v, 0.0)

    l_id = lax.rem(row, N1)
    low = l_id == 0
    face = jnp.logical_and(jnp.logical_or(low, l_id == N1 - 1), row < NODES)
    sign = jnp.where(low, -1.0, 1.0)
    slides = a_id == jnp.where(low, half, half - 1)
    ends = a_id == jnp.where(low, 0, axial - 1)
    for s in range(per_span):
        ln = slice(s * axial, (s + 1) * axial)
        own = [e[f, block, ln] for f in SENT[2]]
        outer = []
        for n, f in enumerate(SENT[2]):
            lo_v = pltpu.roll(e[f, OFF + 4 : OFF + 4 + ROWS, ln], 1, 1)
            hi_v = pltpu.roll(e[f, OFF - 4 : OFF - 4 + ROWS, ln], axial - 1, 1)
            v = jnp.where(slides, own[n], jnp.where(low, lo_v, hi_v))
            outer.append(jnp.where(ends, own[n] if n > 4 else 0.0, v))
        for k, v in enumerate(correction(own, outer, sign, 2)):
            rates[k, :, ln] += jnp.where(face, v, 0.0)

    for k in range(5):
        hi, lo = split(rates[k])
        out[k] = (dot_t(hi, perm[...]) + dot_t(lo, perm[...]))[:NODES]

    def add(side, a, b):
        for at, cond in ((0, side == 0), (last, side == 1)):
            @pl.when(cond)
            def _():
                for k in range(5):
                    out[k, at + a : at + b] += fix[k, : b - a]

    def theta(side, g, copy):
        copy.wait_recv()
        a, b = GROUPS[g]
        at = 7 * a + (g > 0)
        size = 7 * (b - a) + (g == 0)
        th_out[:size] = shuffle(th_recv[side, at : at + size], cross[side])
        own = [th_send[1 - side, at + n * (b - a) : at + (n + 1) * (b - a)] for n in range(7)]
        outer = [th_out[n * (b - a) : (n + 1) * (b - a)] for n in range(7)]
        sgn = jnp.where(side == 0, -1.0, 1.0)
        for k, v in enumerate(correction(own, outer, sgn, 0)):
            fix[k, : b - a] = v
        add(side, a, b)

    def blended(side, g, copy):
        copy.wait_recv()
        a, b = GROUPS[g]
        at = 5 * (a - FIRST)
        there = shuffle(up_recv[side, at : at + 5 * (b - a)], cross[side])
        w = 0.5 * metric_scale[0] / end_weight * jnp.where(side == 0, -1.0, 1.0)
        for k in range(5):
            n = slice(k * (b - a), (k + 1) * (b - a))
            fix[k, : b - a] = w * (up_own[1 - side, at + k * (b - a) : at + (k + 1) * (b - a)] - there[n])
        add(side, a, b)

    theta(far_side, 0, in_near[2][0])
    theta(near_side, 0, in_far[2][0])

    for copy in if_copies:
        copy.wait()
    steps = jnp.where(stator, turn_by, lax.rem(n_blk - turn_by, n_blk))
    chosen = pk[...]
    for k in range(1, n_blk):
        chosen = jnp.where(steps == k, gath[k - 1], chosen)
    chosen = jnp.concatenate([chosen, pltpu.roll(chosen, 64, 1)], axis=0)
    hi, lo = split(chosen)
    parts = dot(turn[...], hi) + dot(turn[...], lo)
    for o in range(8):
        chosen = jnp.where(jnp.logical_and(stator, code == o), parts[o * FROWS : (o + 1) * FROWS], chosen)
    outer = jnp.where(stator, pltpu.roll(chosen, 128 - per_span, 1), pltpu.roll(chosen, per_span, 1))

    def traces(x):
        return [x if n == 0 else pltpu.roll(x, 128 - n * cells, 1) for n in range(7)]

    sgn = jnp.where(stator, 1.0, -1.0)
    for k, v in enumerate(correction(traces(own_face[...]), traces(outer), sgn, 2)):
        at = slice(k * 128, (k + 1) * 128)
        slide[:FROWS, at] = jnp.where(lane < per_span, v, 0.0)
        slide[FROWS:, at] = jnp.where(jnp.logical_and(lane >= per_span, lane < cells), v, 0.0)
    hi, lo = split(slide[...])
    jumps = dot(put[...], hi) + dot(put[...], lo)
    for k in range(5):
        hi, lo = split(jumps[:, k * 128 : (k + 1) * 128])
        out[k] += (dot_t(hi, own_side) + dot_t(lo, own_side))[:NODES]

    mid = pltpu.make_async_copy(out.at[:, 32:96], out_hbm.at[:5, 32:96], saved.at[0])
    mid.start()

    blended(far_side, 1, in_near[3][0])
    for g in (1, 2):
        blended(near_side, g, in_far[3][g - 1])
    blended(far_side, 2, in_near[3][1])

    lows = pltpu.make_async_copy(out.at[:, :32], out_hbm.at[:5, :32], saved.at[1])
    highs = pltpu.make_async_copy(out.at[:, 96:], out_hbm.at[:5, 96:], saved.at[2])
    lows.start()
    highs.start()
    for copy in (near_slot, near_rate, near_full[0], *near_part, far_slot_copy, far_rate, far_full[0], *far_part):
        copy.wait_send()
    for copy in (mid, lows, highs):
        copy.wait()


def finish(stored_in, fields, store, fields_out, store_out, stored, fields_next, store_next, in_sem, f_sem, s_sem):
    count = stored.shape[0]
    loads = [pltpu.make_async_copy(stored_in.at[k], stored.at[k], in_sem.at[k]) for k in range(count)]
    for load in loads:
        load.start()
    saves = []
    for k, load in enumerate(loads):
        load.wait()
        value = section_decay * store[k] + time_step * stored[k]
        store_next[k] = value
        fields_next[k] = fields[k] + section_gain * value
        saves.append(pltpu.make_async_copy(store_next.at[k], store_out.at[k], s_sem.at[k]))
        saves.append(pltpu.make_async_copy(fields_next.at[k], fields_out.at[k], f_sem.at[k]))
        saves[-2].start()
        saves[-1].start()
    for save in saves:
        save.wait()


def on_device(fields, store, mean, sound, slot, turns, offs, n_blk, n_span):
    per_theta, per_span = turns.shape
    assert per_theta == 1 and n_blk % 2 == 0
    elems = slot.shape[0]
    axial = elems // per_span
    w_hi, w_lo = (jnp.asarray(t) for t in derivative_tables())
    pick, turn, put = (jnp.asarray(t) for t in turn_tables())
    vmem = pl.BlockSpec(memory_space=pltpu.VMEM)
    hbm = pl.BlockSpec(memory_space=pl.ANY)
    smem = pl.BlockSpec(memory_space=pltpu.SMEM)
    dma = pltpu.SemaphoreType.DMA
    stored = pl.pallas_call(
        functools.partial(kernel, n_blk, n_span, per_span, axial),
        out_shape=jax.ShapeDtypeStruct((48, NODES, elems), F32),
        in_specs=[hbm] * 3 + [vmem] + [smem] * 2 + [hbm] * 5,
        out_specs=hbm,
        scratch_shapes=[
            pltpu.VMEM(fields.shape, F32),
            pltpu.VMEM((9, OFF + ROWS + 32, elems), F32),
            pltpu.VMEM((elems, elems), BF16),
            pltpu.VMEM((6 * ROWS, 5 * elems), BF16),
            pltpu.VMEM((5, ROWS, elems), F32),
            pltpu.VMEM((2, 7 * FACE + 1, elems), F32),
            pltpu.VMEM((2, 7 * FACE + 1, elems), F32),
            pltpu.VMEM((7 * FACE + 1, elems), F32),
            pltpu.VMEM((2, REST, elems), F32),
            pltpu.VMEM((2, REST, elems), F32),
            pltpu.VMEM((2, 5 * REST, elems), F32),
            pltpu.VMEM((2, 5 * REST, elems), F32),
            pltpu.VMEM((2, 5 * REST, elems), F32),
            pltpu.VMEM((5, FROWS // 2, elems), F32),
            pltpu.VMEM((2, 1, elems), jnp.int32),
            pltpu.VMEM((2, elems, elems), BF16),
            pltpu.VMEM((2, 7, FROWS, axial), F32),
            pltpu.VMEM((2, 7, FROWS, axial), F32),
            pltpu.VMEM((7, ROWS, axial), F32),
            pltpu.VMEM((FROWS // 2, 128), F32),
            pltpu.VMEM((n_blk - 1, FROWS // 2, 128), F32),
            pltpu.VMEM((FROWS, 128), F32),
            pltpu.VMEM((2 * FROWS, 5 * 128), F32),
            pltpu.VMEM(fields.shape, F32),
            pltpu.VMEM(mean.shape, F32),
            pltpu.VMEM(sound.shape, F32),
            *(pltpu.VMEM(t.shape, BF16) for t in (w_hi, w_lo, pick, turn, put)),
            dma((2, len(GROUPS))), dma((2, len(GROUPS))), dma((2,)), dma((2,)), dma((2, 2)), dma((2, 2)),
            dma((2,)), dma((2,)), dma((2,)), dma((2,)),
            dma((n_blk - 1,)), dma((n_blk - 1,)), dma((9,)), dma((3,)),
            pltpu.SemaphoreType.REGULAR, pltpu.SemaphoreType.REGULAR,
        ],
        compiler_params=pltpu.CompilerParams(collective_id=0, has_side_effects=True),
    )(fields, mean, sound, slot.reshape(1, elems), turns, offs, w_hi, w_lo, pick, turn, put)
    shape = jax.ShapeDtypeStruct(fields.shape, F32)
    count = fields.shape[0]
    return pl.pallas_call(
        finish,
        out_shape=(shape, shape),
        in_specs=[hbm, vmem, vmem],
        out_specs=(hbm, hbm),
        scratch_shapes=[pltpu.VMEM(fields.shape, F32)] * 3 + [dma((count,))] * 3,
        compiler_params=pltpu.CompilerParams(vmem_limit_bytes=50 * 2**20),
    )(stored, fields, store)


def solution(mesh):
    whole = P(None, None, ("blk", "span"))
    in_specs = (
        whole, whole, whole, P(None, ("blk", "span")), P(("blk", "span")), P("blk", "span"), P("span"),
    )
    body = functools.partial(on_device, n_blk=mesh.shape["blk"], n_span=mesh.shape["span"])
    return jax.shard_map(
        body, mesh=mesh, in_specs=in_specs, out_specs=(whole, whole), check_vma=False
    )
```
